128 devices in a mesh: replica: 1, data: 128 (over z, y, x, core).
Axes of the slice: x: 4, y: 4, z: 4, core: 2. Of those that a mesh axis runs over, the one named last changes fastest.
Arguments:
- query_hidden: bfloat16 [384, 32, 768], P(('replica', 'data'))
- doc_hidden: bfloat16 [384, 512, 768], P(('replica', 'data'))
- neg_hidden: bfloat16 [384, 4, 512, 768], P(('replica', 'data'))
- query_mask: int32 [384, 32], P(('replica', 'data'))
- doc_mask: int32 [384, 512], P(('replica', 'data'))
- neg_mask: int32 [384, 4, 512], P(('replica', 'data'))
- teacher: float32 [384, 5], P(('replica', 'data'))
- w_proj: bfloat16 [768, 128], replicated
- temperature: float32 [], replicated
Outputs:
- output 1: float32 [384], P(('replica', 'data'))
- output 2: float32 [1], P('replica')
All inputs are finite; a program needn't handle non-finite values.
Results may differ from the reference program's by a relative error of at most 0.001.
Values are sent between devices in bfloat16 or wider.
A program may use at most 1 GiB of HBM per device.

```python
import jax
import jax.numpy as jnp
from jax import lax

BATCH = 384
QUERY_LEN = 32
DOC_LEN = 512
HIDDEN = 768
PROJ_DIM = 128
NUM_HARD = 4


def project_tokens(hidden, w_proj):
    flat_hidden = hidden.reshape(-1, HIDDEN)
    projected = jnp.dot(flat_hidden, w_proj, preferred_element_type=jnp.float32)
    projected = projected / jnp.sqrt(jnp.sum(projected * projected, axis=-1, keepdims=True))
    return projected.astype(jnp.bfloat16).reshape(hidden.shape[:-1] + (PROJ_DIM,))


def prefix_mask(lengths, width):
    return (jnp.arange(width) < lengths[..., None]).astype(jnp.int32)


def setup_inputs(seed: int = 0, part: int = 0) -> dict:
    root_key = jax.random.key(seed)
    key_w, key_temp, key_common, key_part = jax.random.split(root_key, 4)
    part_keys = jax.random.split(jax.random.fold_in(key_part, part), 10)
    common = jax.random.normal(key_common, (HIDDEN,), jnp.float32)
    base_vec = 0.59 * common
    pair_vec = jax.random.normal(part_keys[0], (BATCH, HIDDEN), jnp.float32)
    query_noise = jax.random.normal(part_keys[1], (BATCH, QUERY_LEN, HIDDEN), jnp.float32)
    query_real = base_vec + 0.39 * pair_vec[:, None, :] + 0.71 * query_noise
    copies = -(-DOC_LEN // QUERY_LEN)
    query_tiled = 2.0 * jnp.tile(query_real, (1, copies, 1))[:, :DOC_LEN]
    query_len = jax.random.randint(part_keys[2], (BATCH,), QUERY_LEN // 2, QUERY_LEN + 1, dtype=jnp.int32).at[0].set(QUERY_LEN)
    doc_len = jax.random.randint(part_keys[3], (BATCH,), DOC_LEN // 4, DOC_LEN + 1, dtype=jnp.int32).at[0].set(DOC_LEN)
    neg_len = jax.random.randint(part_keys[4], (BATCH, NUM_HARD), DOC_LEN // 4, DOC_LEN + 1, dtype=jnp.int32).at[0, 0].set(DOC_LEN)
    query_mask = prefix_mask(query_len, QUERY_LEN)
    doc_mask = prefix_mask(doc_len, DOC_LEN)
    neg_mask = prefix_mask(neg_len, DOC_LEN)
    doc_noise = jax.random.normal(part_keys[5], (BATCH, DOC_LEN, HIDDEN), jnp.float32)
    doc_real = base_vec + 0.39 * pair_vec[:, None, :] + 0.71 * doc_noise
    doc_hidden = jnp.where(doc_mask[:, :, None] > 0, doc_real, query_tiled + 0.3 * doc_noise)
    neg_share = jax.random.uniform(part_keys[6], (BATCH, NUM_HARD, 1, 1), jnp.float32, minval=0.4, maxval=0.9)
    neg_vec = jax.random.normal(part_keys[7], (BATCH, NUM_HARD, 1, HIDDEN), jnp.float32)
    neg_mix = neg_share * pair_vec[:, None, None, :] + jnp.sqrt(1.0 - neg_share * neg_share) * neg_vec
    neg_noise = jax.random.normal(part_keys[8], (BATCH, NUM_HARD, DOC_LEN, HIDDEN), jnp.float32)
    neg_real = base_vec + 0.39 * neg_mix + 0.71 * neg_noise
    neg_hidden = jnp.where(neg_mask[..., None] > 0, neg_real, query_tiled[:, None] + 0.3 * neg_noise)
    teacher = jax.random.normal(part_keys[9], (BATCH, NUM_HARD + 1), jnp.float32).at[:, 0].add(2.0)
    w_proj = jax.random.normal(key_w, (HIDDEN, PROJ_DIM), jnp.float32) * HIDDEN ** -0.5
    temperature = QUERY_LEN * jax.random.uniform(key_temp, (), jnp.float32, minval=0.04, maxval=0.07)
    return {
        'query_hidden': query_real.astype(jnp.bfloat16),
        'doc_hidden': doc_hidden.astype(jnp.bfloat16),
        'neg_hidden': neg_hidden.astype(jnp.bfloat16),
        'query_mask': query_mask,
        'doc_mask': doc_mask,
        'neg_mask': neg_mask,
        'teacher': teacher,
        'w_proj': w_proj.astype(jnp.bfloat16),
        'temperature': temperature,
    }


def reference(query_hidden, doc_hidden, neg_hidden, query_mask, doc_mask, neg_mask, teacher, w_proj, temperature):
    query_tok = project_tokens(query_hidden, w_proj).astype(jnp.float32)
    doc_tok = project_tokens(doc_hidden, w_proj).astype(jnp.float32)
    neg_tok = project_tokens(neg_hidden, w_proj).astype(jnp.float32)
    query_weight = query_mask.astype(jnp.float32)
    doc_valid = doc_mask > 0

    def score_query(query_item):
        query_rows, row_weight, neg_rows, neg_valid = query_item
        sim_tile = jnp.einsum('td,jsd->tjs', query_rows, doc_tok)
        best_sim = jnp.max(jnp.where(doc_valid[None], sim_tile, -jnp.inf), axis=2)
        in_batch = jnp.sum(row_weight[:, None] * best_sim, axis=0)
        hard_sim = jnp.einsum('td,ksd->tks', query_rows, neg_rows)
        hard_best = jnp.max(jnp.where(neg_valid[None] > 0, hard_sim, -jnp.inf), axis=2)
        hard_row = jnp.sum(row_weight[:, None] * hard_best, axis=0)
        return in_batch, hard_row

    scores, hard_scores = lax.map(score_query, (query_tok, query_weight, neg_tok, neg_mask))
    logits = scores / temperature
    positive = jnp.diagonal(logits)
    cross_ent = jax.nn.logsumexp(logits, axis=1) - positive
    student = jnp.concatenate([positive[:, None], hard_scores / temperature], axis=1)
    student_log = jax.nn.log_softmax(student, axis=1)
    teacher_log = jax.nn.log_softmax(teacher, axis=1)
    kl_div = jnp.sum(jnp.exp(teacher_log) * (teacher_log - student_log), axis=1)
    loss_rows = cross_ent + kl_div
    return loss_rows, jnp.mean(loss_rows, keepdims=True)
```

```python
import functools

import jax
import jax.numpy as jnp
from jax import lax
from jax.experimental import pallas as pl
from jax.experimental.pallas import tpu as pltpu
from jax.sharding import PartitionSpec as P

RING = 4
CHIPS = RING ** 3
PLANE = RING * RING
ORDERS = ((0, 1, 2), (1, 2, 0), (2, 0, 1))
UNITS = 16
LOW = -3.0e38


def kernel(qh, dh, nh, qm, dm, nm, te, w, tau_ref, loss_ref, mean_ref,
           qv, dv, nv, qmv, dmv, nmv, tev, wv, gath, docs, best, hard, part, inbox, tot, totin,
           in_sem, doc_sem, gsend, grecv, psend, precv, tsem):
    me = lax.axis_index('data')
    core = lax.rem(me, 2)
    chip = me // 2
    pos = (lax.rem(chip, RING), lax.rem(chip // RING, RING), chip // PLANE)
    nq, dlen = dv.shape[0], dv.shape[1]
    nneg = nv.shape[1]
    qlen = qv.shape[1]

    def device(axis, off):
        c = list(pos)
        c[axis] = lax.rem(pos[axis] + off, RING)
        return {'data': ((c[2] * RING + c[1]) * RING + c[0]) * 2 + core}

    partner = {'data': chip * 2 + 1 - core}

    loads = [pltpu.make_async_copy(w, wv, in_sem.at[0]),
             pltpu.make_async_copy(qh, qv, in_sem.at[1]),
             pltpu.make_async_copy(qm, qmv, in_sem.at[2]),
             pltpu.make_async_copy(dm, dmv, in_sem.at[3]),
             pltpu.make_async_copy(nm, nmv, in_sem.at[4]),
             pltpu.make_async_copy(te, tev, in_sem.at[5])]
    doc_loads = [pltpu.make_async_copy(dh.at[j], dv.at[j], in_sem.at[6 + j]) for j in range(nq)]
    neg_loads = [pltpu.make_async_copy(nh.at[i], nv.at[i], in_sem.at[6 + nq + i]) for i in range(nq)]
    for load in loads + doc_loads + neg_loads:
        load.start()

    barrier = pltpu.get_barrier_semaphore()
    for axis in range(3):
        for off in range(1, RING):
            pl.semaphore_signal(barrier, inc=1, device_id=device(axis, off), device_id_type=pl.DeviceIdType.MESH)
    pl.semaphore_signal(barrier, inc=1, device_id=partner, device_id_type=pl.DeviceIdType.MESH)

    def project(rows):
        y = jnp.dot(rows, wv[...], preferred_element_type=jnp.float32)
        return y * lax.rsqrt(jnp.sum(y * y, axis=-1, keepdims=True))

    def length(mask_row):
        return jnp.sum(mask_row.astype(jnp.float32), axis=-1, keepdims=True)

    def row_ids(rows, cols):
        return lax.broadcasted_iota(jnp.int32, (rows, cols), 0).astype(jnp.float32)

    hard[...] = jnp.zeros_like(hard)
    best[...] = jnp.zeros_like(best)
    for load in loads:
        load.wait()

    own = []
    for q in range(nq):
        a1, a2, a3 = ORDERS[q]
        own.append((pos[a3] * RING + pos[a2]) * RING + pos[a1])
        tok = project(qv[q])
        keep = row_ids(qlen, tok.shape[1]) < length(qmv[q:q + 1, :])
        gath[q, own[q]] = jnp.where(keep, tok, 0.0).astype(jnp.bfloat16)

    pl.semaphore_wait(barrier, 3 * (RING - 1) + 1)

    def copies(stage, q):
        axis = ORDERS[q][stage]
        span = RING ** stage
        a1, a2, a3 = ORDERS[q]
        out = []
        for off in range(1, RING):
            def start_of(shift):
                c = list(pos)
                c[axis] = lax.rem(pos[axis] + shift, RING)
                flat = (c[a3] * RING + c[a2]) * RING + c[a1]
                return flat if span == 1 else (flat // span) * span
            mine = gath.at[q, pl.ds(start_of(0), span)]
            theirs = gath.at[q, pl.ds(start_of(RING - off), span)]
            send = pltpu.make_async_remote_copy(
                src_ref=mine, dst_ref=mine, send_sem=gsend.at[stage, q, off - 1], recv_sem=grecv.at[stage, q, off - 1],
                device_id=device(axis, off), device_id_type=pl.DeviceIdType.MESH)
            recv = pltpu.make_async_remote_copy(
                src_ref=theirs, dst_ref=theirs, send_sem=gsend.at[stage, q, off - 1],
                recv_sem=grecv.at[stage, q, off - 1],
                device_id=device(axis, off), device_id_type=pl.DeviceIdType.MESH)
            out.append((send, recv))
        return out

    gather = [[copies(stage, q) for q in range(nq)] for stage in range(3)]

    for q in range(nq):
        for send, _ in gather[0][q]:
            send.start()

    def valid_rows(y, mask_row):
        keep = row_ids(dlen, y.shape[1]) < length(mask_row)
        return jnp.where(keep, y, y[0:1, :]).astype(jnp.bfloat16)

    for j in range(nq):
        doc_loads[j].wait()
        docs[core * nq + j] = valid_rows(project(dv[j]), dmv[j:j + 1, :])

    my_docs = docs.at[pl.ds(core * nq, nq)]
    their_docs = docs.at[pl.ds((1 - core) * nq, nq)]
    doc_send = pltpu.make_async_remote_copy(
        src_ref=my_docs, dst_ref=my_docs, send_sem=doc_sem.at[0], recv_sem=doc_sem.at[1],
        device_id=partner, device_id_type=pl.DeviceIdType.MESH)
    doc_recv = pltpu.make_async_remote_copy(
        src_ref=their_docs, dst_ref=their_docs, send_sem=doc_sem.at[0], recv_sem=doc_sem.at[1],
        device_id=partner, device_id_type=pl.DeviceIdType.MESH)
    contract = (((1,), (1,)), ((), ()))
    cell_row = lax.broadcasted_iota(jnp.int32, hard.shape, 0)
    cell_lane = lax.broadcasted_iota(jnp.int32, hard.shape, 1)

    def negatives(i):
        neg_loads[i].wait()
        mine = gath[i, own[i]]
        for k in range(nneg):
            tok = valid_rows(project(nv[i, k]), nmv[i, k:k + 1, :])
            sim = lax.dot_general(tok, mine, contract, preferred_element_type=jnp.float32)
            score = jnp.sum(jnp.max(sim, axis=0, keepdims=True), axis=1, keepdims=True)
            hard[...] = jnp.where((cell_row == i) & (cell_lane == k + 1), score, hard[...])

    def forward(stage):
        for q in range(nq):
            for _, recv in gather[stage - 1][q]:
                recv.wait_recv()
            for send, _ in gather[stage][q]:
                send.start()

    negatives(0)
    doc_send.start()
    forward(1)
    negatives(1)
    forward(2)
    negatives(2)
    doc_recv.wait_recv()

    unit_row = lax.broadcasted_iota(jnp.int32, (8, PLANE * qlen), 0)

    def score_unit(q, plane):
        rows = gath[q, pl.ds(plane * PLANE, PLANE)].reshape(PLANE * qlen, gath.shape[3])
        unit = jnp.zeros((8, PLANE * qlen), jnp.float32)
        for j in range(2 * nq):
            halves = []
            for h in range(PLANE * qlen // 256):
                sim = lax.dot_general(docs[j], rows[h * 256:(h + 1) * 256], contract,
                                      preferred_element_type=jnp.float32)
                halves.append(jnp.max(sim, axis=0, keepdims=True))
            unit = jnp.where(unit_row == j, jnp.concatenate(halves, axis=1), unit)
        best[q * RING + plane] = unit

    for q in range(nq):
        score_unit(q, pos[ORDERS[q][2]])
    for off in (1, 3, 2):
        for q in range(nq):
            gather[2][q][off - 1][1].wait_recv()
            score_unit(q, lax.rem(pos[ORDERS[q][2]] + RING - off, RING))

    tau = tau_ref[0]
    flat = best[...].reshape(UNITS * 8, PLANE * qlen)
    first = lax.broadcasted_iota(jnp.int32, (PLANE * qlen, 128), 1) * qlen
    token = lax.broadcasted_iota(jnp.int32, (PLANE * qlen, 128), 0)
    ones = jnp.where((token >= first) & (token < first + qlen), 1.0, 0.0)
    scores = lax.dot_general(flat, ones, (((1,), (0,)), ((), ())), precision=lax.Precision.HIGHEST,
                             preferred_element_type=jnp.float32).reshape(UNITS, 8, 128)
    u_id = lax.broadcasted_iota(jnp.int32, (UNITS, 8, 128), 0)
    j_id = lax.broadcasted_iota(jnp.int32, (UNITS, 8, 128), 1)
    l_id = lax.broadcasted_iota(jnp.int32, (UNITS, 8, 128), 2)

    students = hard[...]
    for q in range(nq):
        a1, a2, a3 = ORDERS[q]
        here = (u_id == q * RING + pos[a3]) & (j_id == core * nq + q) & (l_id == pos[a2] * RING + pos[a1])
        hit = jnp.sum(jnp.where(here, scores, 0.0), axis=0)
        hit = jnp.sum(jnp.sum(hit, axis=0, keepdims=True), axis=1, keepdims=True)
        students = jnp.where((cell_row == q) & (cell_lane == 0), hit, students)

    def log_softmax(z):
        z = z - jnp.max(z, axis=1, keepdims=True)
        return z - jnp.log(jnp.sum(jnp.exp(z), axis=1, keepdims=True))

    logits = students[:nq, :nneg + 1] / tau
    teacher_log = log_softmax(tev[...])
    student_log = log_softmax(logits)
    rest = jnp.sum(jnp.exp(teacher_log) * (teacher_log - student_log), axis=1, keepdims=True) - logits[:, 0:1]
    rest_sum = jnp.sum(rest, axis=0, keepdims=True)

    real = j_id < 2 * nq
    top = jnp.max(jnp.where(real, scores, LOW), axis=1, keepdims=True)
    mass = jnp.sum(jnp.where(real, jnp.exp((scores - top) / tau), 0.0), axis=1)
    top = top.reshape(UNITS, 128)
    p_row = lax.broadcasted_iota(jnp.int32, (UNITS, 128), 0)
    p_lane = lax.broadcasted_iota(jnp.int32, (UNITS, 128), 1)
    used = p_row < nq * RING
    mass = jnp.where(used, mass, jnp.where((p_row == nq * RING) & (p_lane == 0), rest_sum, 0.0))
    top = jnp.where(used, top, 0.0)

    for stage in range(3):
        part[stage, 0] = top
        part[stage, 1] = mass
        moves = []
        for off in range(1, RING):
            move = pltpu.make_async_remote_copy(
                src_ref=part.at[stage], dst_ref=inbox.at[stage, off - 1], send_sem=psend.at[stage, off - 1],
                recv_sem=precv.at[stage, off - 1], device_id=device(stage, off),
                device_id_type=pl.DeviceIdType.MESH)
            move.start()
            moves.append(move)
        for move in moves:
            move.wait()
        tops = [top] + [inbox[stage, o, 0] for o in range(RING - 1)]
        masses = [mass] + [inbox[stage, o, 1] for o in range(RING - 1)]
        top = functools.reduce(jnp.maximum, tops)
        mass = sum(ms * jnp.exp((tp - top) / tau) for tp, ms in zip(tops, masses))

    lse = jnp.where(used & (p_lane < PLANE), top / tau + jnp.log(jnp.where(used, mass, 1.0)), 0.0)
    extra = jnp.where((p_row == nq * RING) & (p_lane == 0), mass, 0.0)
    mine = jnp.sum(jnp.sum(lse + extra, axis=0, keepdims=True), axis=1, keepdims=True)
    tot[...] = jnp.broadcast_to(mine, tot.shape)
    swap = pltpu.make_async_remote_copy(
        src_ref=tot, dst_ref=totin, send_sem=tsem.at[0], recv_sem=tsem.at[1],
        device_id=partner, device_id_type=pl.DeviceIdType.MESH)
    swap.start()
    rest_row = lax.broadcasted_iota(jnp.int32, rest.shape, 0)
    for q in range(nq):
        a1, a2, a3 = ORDERS[q]
        here = (p_row == q * RING + pos[a3]) & (p_lane == pos[a2] * RING + pos[a1])
        loss_ref[q] = jnp.sum(jnp.where(here, lse, 0.0)) + jnp.sum(jnp.where(rest_row == q, rest, 0.0))
    swap.wait()
    mean_ref[0] = jnp.sum((tot[0:1, 0:1] + totin[0:1, 0:1]) / (2 * CHIPS * nq))

    doc_send.wait_send()
    for stage in range(3):
        for q in range(nq):
            for send, _ in gather[stage][q]:
                send.wait_send()


def solution(mesh):
    batch_axes = ('replica', 'data')

    def local_loss(query_hidden, doc_hidden, neg_hidden, query_mask, doc_mask, neg_mask, teacher, w_proj, temperature):
        nq, qlen, width = query_hidden.shape
        dlen, nneg = doc_hidden.shape[1], neg_hidden.shape[1]
        proj = w_proj.shape[1]
        anywhere = pl.BlockSpec(memory_space=pl.ANY)
        smem = pl.BlockSpec(memory_space=pltpu.SMEM)
        rows = nq * (qlen + dlen + nneg * dlen)
        loss, mean = pl.pallas_call(
            kernel,
            name='late_interaction',
            out_shape=(jax.ShapeDtypeStruct((nq,), jnp.float32), jax.ShapeDtypeStruct((1,), jnp.float32)),
            in_specs=[anywhere] * 8 + [smem],
            out_specs=(smem, smem),
            scratch_shapes=[
                pltpu.VMEM(query_hidden.shape, jnp.bfloat16),
                pltpu.VMEM(doc_hidden.shape, jnp.bfloat16),
                pltpu.VMEM(neg_hidden.shape, jnp.bfloat16),
                pltpu.VMEM(query_mask.shape, jnp.int32),
                pltpu.VMEM(doc_mask.shape, jnp.int32),
                pltpu.VMEM(neg_mask.shape, jnp.int32),
                pltpu.VMEM(teacher.shape, jnp.float32),
                pltpu.VMEM(w_proj.shape, jnp.bfloat16),
                pltpu.VMEM((nq, CHIPS, qlen, proj), jnp.bfloat16),
                pltpu.VMEM((2 * nq, dlen, proj), jnp.bfloat16),
                pltpu.VMEM((UNITS, 8, PLANE * qlen), jnp.float32),
                pltpu.VMEM((8, 128), jnp.float32),
                pltpu.VMEM((3, 2, UNITS, 128), jnp.float32),
                pltpu.VMEM((3, RING - 1, 2, UNITS, 128), jnp.float32),
                pltpu.VMEM((8, 128), jnp.float32),
                pltpu.VMEM((8, 128), jnp.float32),
                pltpu.SemaphoreType.DMA((6 + 2 * nq,)),
                pltpu.SemaphoreType.DMA((2,)),
                pltpu.SemaphoreType.DMA((3, nq, RING - 1)),
                pltpu.SemaphoreType.DMA((3, nq, RING - 1)),
                pltpu.SemaphoreType.DMA((3, RING - 1)),
                pltpu.SemaphoreType.DMA((3, RING - 1)),
                pltpu.SemaphoreType.DMA((2,)),
            ],
            compiler_params=pltpu.CompilerParams(
                collective_id=0, has_side_effects=True, vmem_limit_bytes=60 * 1024 * 1024),
            cost_estimate=pl.CostEstimate(
                flops=2 * proj * (rows * width + CHIPS * nq * qlen * 2 * nq * dlen),
                bytes_accessed=2 * rows * width, transcendentals=rows),
        )(query_hidden, doc_hidden, neg_hidden, query_mask, doc_mask, neg_mask, teacher, w_proj,
          temperature.reshape(1))
        return loss, mean

    in_specs = (P(batch_axes, None, None), P(batch_axes, None, None), P(batch_axes, None, None, None),
                P(batch_axes, None), P(batch_axes, None), P(batch_axes, None, None), P(batch_axes, None),
                P(None, None), P())
    out_specs = (P(batch_axes), P('replica'))
    return jax.shard_map(local_loss, mesh=mesh, in_specs=in_specs, out_specs=out_specs, check_vma=False)
```

```python
import jax
import jax.numpy as jnp
from jax import lax
from jax.experimental import pallas as pl
from jax.experimental.pallas import tpu as pltpu
from jax.sharding import PartitionSpec as P

RING = 4
CHIPS = RING ** 3
ORDERS = ((0, 1, 2), (1, 2, 0), (2, 0, 1))
SLOTS = ((0, 0), (0, 1), (0, 3), (0, 2), (1, 0), (3, 0), (2, 0), (1, 1),
         (3, 1), (2, 1), (1, 3), (3, 3), (2, 3), (1, 2), (3, 2), (2, 2))
NEAR_FIRST = (1, 3, 2)
OTHERS = sorted([(x, y, z) for x in range(RING) for y in range(RING) for z in range(RING) if x or y or z],
                key=lambda v: -sum(min(a, RING - a) for a in v))
LOW = -3.0e38
MESH = pl.DeviceIdType.MESH


def kernel(qh, dh, nh, qm, dm, nm, te, w, tau_ref, loss_ref, mean_ref,
           qv, dv, nv, qmv, dmv, nmv, tev, wv, gath, docs, best, hard, ones, dense, rest_ref, inbox, tot, totin,
           in_sem, doc_sem, gsend, grecv, osend, orecv, tsem):
    me = lax.axis_index('data')
    core = lax.rem(me, 2)
    chip = me // 2
    pos = (lax.rem(chip, RING), lax.rem(chip // RING, RING), chip // (RING * RING))
    nq, dlen, width = dv.shape
    nneg, qlen, proj = nv.shape[1], qv.shape[1], wv.shape[1]
    tau = tau_ref[0]

    def device(steps):
        c = [lax.rem(pos[a] + steps[a], RING) if steps[a] else pos[a] for a in range(3)]
        return {'data': ((c[2] * RING + c[1]) * RING + c[0]) * 2 + core}

    def along(axis, off):
        return device([off if a == axis else 0 for a in range(3)])

    partner = {'data': chip * 2 + 1 - core}

    def remote(src, dst, send, recv, target):
        return pltpu.make_async_remote_copy(src_ref=src, dst_ref=dst, send_sem=send, recv_sem=recv,
                                            device_id=target, device_id_type=MESH)

    pairs = ((w, wv), (qh, qv), (qm, qmv), (dm, dmv), (nm, nmv), (te, tev))
    loads = [pltpu.make_async_copy(src, dst, in_sem.at[n]) for n, (src, dst) in enumerate(pairs)]
    first, small = loads[:3], loads[3:]
    doc_loads = [pltpu.make_async_copy(dh.at[j], dv.at[j], in_sem.at[6 + j]) for j in range(nq)]
    neg_loads = [pltpu.make_async_copy(nh.at[i], nv.at[i], in_sem.at[6 + nq + i]) for i in range(nq)]
    for load in first + small + doc_loads + neg_loads:
        load.start()

    barrier = pltpu.get_barrier_semaphore()
    for axis in range(3):
        for off in range(1, RING):
            pl.semaphore_signal(barrier, inc=1, device_id=along(axis, off), device_id_type=MESH)
    pl.semaphore_signal(barrier, inc=1, device_id=partner, device_id_type=MESH)

    def project(rows):
        y = jnp.dot(rows, wv[...], preferred_element_type=jnp.float32)
        return y * lax.rsqrt(jnp.sum(y * y, axis=-1, keepdims=True))

    def length(mask_row):
        return jnp.sum(mask_row.astype(jnp.float32), axis=-1, keepdims=True)

    def row_ids(rows, cols):
        return lax.broadcasted_iota(jnp.int32, (rows, cols), 0).astype(jnp.float32)

    hard[...] = jnp.zeros_like(hard)
    dense[...] = jnp.zeros_like(dense)
    e_row = lax.broadcasted_iota(jnp.int32, ones.shape, 0)
    e_lane = lax.rem(lax.broadcasted_iota(jnp.int32, ones.shape, 1), RING) * qlen
    ones[...] = jnp.where((e_row >= e_lane) & (e_row < e_lane + qlen), 1.0, 0.0)

    for load in first:
        load.wait()
    for q in range(nq):
        tok = project(qv[q])
        keep = row_ids(qlen, proj) < length(qmv[q:q + 1, :])
        gath[q * RING + pos[ORDERS[q][0]]] = jnp.where(keep, tok, 0.0).astype(jnp.bfloat16)

    pl.semaphore_wait(barrier, 3 * (RING - 1) + 1)

    slot_of = {pair: n for n, pair in enumerate(SLOTS)}

    for off in NEAR_FIRST:
        for q in range(nq):
            a1 = ORDERS[q][0]
            block = gath.at[q * RING + pos[a1]]
            remote(block, block, gsend, grecv.at[0], along(a1, off)).start()

    def row_of(n, q):
        return gath.at[pl.ds((n * nq + q) * RING, RING)]

    def send_row(r, level):
        for off in NEAR_FIRST:
            back = (0, RING - off) if level == 1 else (RING - off, r)
            for q in range(nq):
                n = slot_of[back]
                remote(row_of(slot_of[(0, r)], q), row_of(n, q), gsend, grecv.at[n],
                       along(ORDERS[q][level], off)).start()

    def arrived(n):
        part = gath.at[pl.ds(n * nq * RING, nq * RING if n else nq * (RING - 1))]
        remote(part, part, gsend, grecv.at[n], partner).wait_recv()

    for load in small:
        load.wait()

    def valid_rows(y, mask_row):
        keep = row_ids(dlen, proj) < length(mask_row)
        return jnp.where(keep, y, y[0:1, :]).astype(jnp.bfloat16)

    for j in range(nq):
        doc_loads[j].wait()
        docs[core * nq + j] = valid_rows(project(dv[j]), dmv[j:j + 1, :])

    my_docs = docs.at[pl.ds(core * nq, nq)]
    their_docs = docs.at[pl.ds((1 - core) * nq, nq)]
    doc_send = remote(my_docs, my_docs, doc_sem.at[0], doc_sem.at[1], partner)
    doc_recv = remote(their_docs, their_docs, doc_sem.at[0], doc_sem.at[1], partner)
    contract = (((1,), (1,)), ((), ()))
    cell_row = lax.broadcasted_iota(jnp.int32, (8, proj), 0)
    cell_lane = lax.broadcasted_iota(jnp.int32, (8, proj), 1)
    cell = cell_row * (proj // RING) + cell_lane // RING

    def negative(i, k):
        if k == 0:
            neg_loads[i].wait()
        mine = gath[i * RING + pos[ORDERS[i][0]]]
        tok = valid_rows(project(nv[i, k]), nmv[i, k:k + 1, :])
        sim = lax.dot_general(tok, mine, contract, preferred_element_type=jnp.float32)
        score = jnp.sum(jnp.max(sim, axis=0, keepdims=True), axis=1, keepdims=True)
        hard[...] = jnp.where((cell_row == i) & (cell_lane == k + 1), score, hard[...])

    def place(q, i3, i2):
        a1, a2, a3 = ORDERS[q]
        return (q * RING + lax.rem(pos[a3] + i3, RING)) * RING + lax.rem(pos[a2] + i2, RING)

    pieces = 2 * nq
    tile = 2 * proj
    tile_row = lax.broadcasted_iota(jnp.int32, (8, tile), 0)

    def segment(s):
        rows = gath[s * pieces * RING:(s + 1) * pieces * RING].reshape(pieces * RING * qlen, proj)
        for t in range(pieces * RING * qlen // tile):
            unit = jnp.zeros((8, tile), jnp.float32)
            for j in range(2 * nq):
                sim = lax.dot_general(docs[j], rows[t * tile:(t + 1) * tile], contract,
                                      preferred_element_type=jnp.float32)
                unit = jnp.where(tile_row == j, jnp.max(sim, axis=0, keepdims=True), unit)
            best[s % 2, 2 * t] = unit[:, :proj]
            best[s % 2, 2 * t + 1] = unit[:, proj:]

    def reduce_segment(s):
        flat = best[s % 2].reshape(pieces * 8, proj)
        scores = lax.dot_general(flat, ones[...], (((1,), (0,)), ((), ())), precision=lax.Precision.HIGHEST,
                                 preferred_element_type=jnp.float32).reshape(pieces, 8, proj)
        real = lax.broadcasted_iota(jnp.int32, scores.shape, 1) < 2 * nq
        top = jnp.max(jnp.where(real, scores, LOW), axis=1, keepdims=True)
        mass = jnp.sum(jnp.where(real, jnp.exp((scores - top) / tau), 0.0), axis=1, keepdims=True)
        part = top / tau + jnp.log(mass)
        packed = dense[...]
        for p in range(pieces):
            i3, i2 = SLOTS[2 * s + p // nq]
            packed = jnp.where(cell == place(p % nq, i3, i2), part[p], packed)
        dense[...] = packed
        if s == 0:
            students = hard[...]
            for q in range(nq):
                here = (cell_row == core * nq + q) & (cell_lane == pos[ORDERS[q][0]])
                hit = jnp.sum(jnp.where(here, scores[q], 0.0), axis=0, keepdims=True)
                hit = jnp.sum(hit, axis=1, keepdims=True)
                students = jnp.where((cell_row == q) & (cell_lane == 0), hit, students)
            hard[...] = students

    def log_softmax(z):
        z = z - jnp.max(z, axis=1, keepdims=True)
        return z - jnp.log(jnp.sum(jnp.exp(z), axis=1, keepdims=True))

    def finish_rows():
        logits = hard[:nq, :nneg + 1] / tau
        teacher_log = log_softmax(tev[...])
        student_log = log_softmax(logits)
        rest = jnp.sum(jnp.exp(teacher_log) * (teacher_log - student_log), axis=1, keepdims=True) - logits[:, 0:1]
        rest_ref[...] = jnp.broadcast_to(rest, rest_ref.shape)
        rest_sum = jnp.sum(rest, axis=0, keepdims=True)
        dense[...] = jnp.where((cell_row == 1) & (cell_lane == proj - 1), rest_sum, dense[...])

    negative(0, 0)
    doc_send.start()
    for n in range(1, 6):
        negative(n // nneg, n % nneg)
    arrived(0)
    send_row(0, 1)
    send_row(0, 2)
    for n in range(6, nq * nneg):
        negative(n // nneg, n % nneg)
    doc_recv.wait_recv()
    for r in (1, 3, 2):
        arrived(slot_of[(0, r)])
        send_row(r, 2)
    for s in range(len(SLOTS) // 2):
        for n in (2 * s, 2 * s + 1):
            if SLOTS[n][0]:
                arrived(n)
        if s:
            reduce_segment(s - 1)
        if s == 2:
            finish_rows()
        segment(s)
    reduce_segment(len(SLOTS) // 2 - 1)

    inbox[chip] = dense[0:2, :]
    mine = inbox.at[chip]
    for steps in OTHERS:
        remote(mine, mine, osend, orecv, device(steps)).start()
    others = inbox.at[pl.ds(0, CHIPS - 1)]
    remote(others, others, osend, orecv, partner).wait_recv()

    parts = inbox[...]
    top = jnp.max(parts, axis=0)
    lse = top + jnp.log(jnp.sum(jnp.exp(parts - top[None]), axis=0))
    r_id = lax.broadcasted_iota(jnp.int32, (2, proj), 0)
    l_id = lax.broadcasted_iota(jnp.int32, (2, proj), 1)
    r_cell = r_id * (proj // RING) + l_id // RING
    extra = jnp.where((r_id == 1) & (l_id == proj - 1), jnp.sum(parts, axis=0), 0.0)
    total = jnp.where(r_cell < nq * RING * RING, lse, extra)
    total = jnp.sum(jnp.sum(total, axis=0, keepdims=True), axis=1, keepdims=True)
    tot[...] = jnp.broadcast_to(total, tot.shape)
    swap = remote(tot, totin, tsem.at[0], tsem.at[1], partner)
    swap.start()
    for q in range(nq):
        here = (r_cell == place(q, 0, 0)) & (lax.rem(l_id, RING) == pos[ORDERS[q][0]])
        loss_ref[q] = jnp.sum(jnp.where(here, lse, 0.0)) + jnp.sum(rest_ref[q:q + 1, 0:1])
    swap.wait()
    mean_ref[0] = jnp.sum((tot[0:1, 0:1] + totin[0:1, 0:1]) / (2 * CHIPS * nq))

    doc_send.wait_send()
    remote(others, others, osend, orecv, partner).wait_send()
    sent = gath.at[pl.ds(0, nq * (RING - 1) + (len(SLOTS) - 1) * nq * RING)]
    remote(sent, sent, gsend, grecv.at[0], partner).wait_send()


def solution(mesh):
    batch_axes = ('replica', 'data')

    def local_loss(query_hidden, doc_hidden, neg_hidden, query_mask, doc_mask, neg_mask, teacher, w_proj, temperature):
        nq, qlen, width = query_hidden.shape
        dlen, nneg = doc_hidden.shape[1], neg_hidden.shape[1]
        proj = w_proj.shape[1]
        anywhere = pl.BlockSpec(memory_space=pl.ANY)
        smem = pl.BlockSpec(memory_space=pltpu.SMEM)
        rows = nq * (qlen + dlen + nneg * dlen)
        loss, mean = pl.pallas_call(
            kernel,
            name='late_interaction',
            out_shape=(jax.ShapeDtypeStruct((nq,), jnp.float32), jax.ShapeDtypeStruct((1,), jnp.float32)),
            in_specs=[anywhere] * 8 + [smem],
            out_specs=(smem, smem),
            scratch_shapes=[
                pltpu.VMEM(query_hidden.shape, jnp.bfloat16),
                pltpu.VMEM(doc_hidden.shape, jnp.bfloat16),
                pltpu.VMEM(neg_hidden.shape, jnp.bfloat16),
                pltpu.VMEM(query_mask.shape, jnp.int32),
                pltpu.VMEM(doc_mask.shape, jnp.int32),
                pltpu.VMEM(neg_mask.shape, jnp.int32),
                pltpu.VMEM(teacher.shape, jnp.float32),
                pltpu.VMEM(w_proj.shape, jnp.bfloat16),
                pltpu.VMEM((len(SLOTS) * nq * RING, qlen, proj), jnp.bfloat16),
                pltpu.VMEM((2 * nq, dlen, proj), jnp.bfloat16),
                pltpu.VMEM((2, 2 * nq, 8, proj), jnp.float32),
                pltpu.VMEM((8, proj), jnp.float32),
                pltpu.VMEM((proj, proj), jnp.float32),
                pltpu.VMEM((8, proj), jnp.float32),
                pltpu.VMEM((nq, proj), jnp.float32),
                pltpu.VMEM((CHIPS, 2, proj), jnp.float32),
                pltpu.VMEM((1, proj), jnp.float32),
                pltpu.VMEM((1, proj), jnp.float32),
                pltpu.SemaphoreType.DMA((6 + 2 * nq,)),
                pltpu.SemaphoreType.DMA((2,)),
                pltpu.SemaphoreType.DMA,
                pltpu.SemaphoreType.DMA((len(SLOTS),)),
                pltpu.SemaphoreType.DMA,
                pltpu.SemaphoreType.DMA,
                pltpu.SemaphoreType.DMA((2,)),
            ],
            compiler_params=pltpu.CompilerParams(
                collective_id=0, has_side_effects=True, vmem_limit_bytes=60 * 1024 * 1024),
            cost_estimate=pl.CostEstimate(
                flops=2 * proj * (rows * width + CHIPS * nq * qlen * 2 * nq * dlen),
                bytes_accessed=2 * rows * width, transcendentals=rows),
        )(query_hidden, doc_hidden, neg_hidden, query_mask, doc_mask, neg_mask, teacher, w_proj,
          temperature.reshape(1))
        return loss, mean

    in_specs = (P(batch_axes, None, None), P(batch_axes, None, None), P(batch_axes, None, None, None),
                P(batch_axes, None), P(batch_axes, None), P(batch_axes, None, None), P(batch_axes, None),
                P(None, None), P())
    out_specs = (P(batch_axes), P('replica'))
    return jax.shard_map(local_loss, mesh=mesh, in_specs=in_specs, out_specs=out_specs, check_vma=False)
```

```python
import jax
import jax.numpy as jnp
from jax import lax
from jax.experimental import pallas as pl
from jax.experimental.pallas import tpu as pltpu
from jax.sharding import PartitionSpec as P

RING = 4
CHIPS = RING ** 3
ORDERS = ((0, 1, 2), (1, 2, 0), (2, 0, 1))
SLOTS = ((0, 0), (0, 1), (0, 3), (0, 2), (1, 0), (3, 0), (2, 0), (1, 1),
         (3, 1), (2, 1), (1, 3), (3, 3), (2, 3), (1, 2), (3, 2), (2, 2))
NEAR_FIRST = (1, 3, 2)
OTHERS = sorted([(x, y, z) for x in range(RING) for y in range(RING) for z in range(RING) if x or y or z],
                key=lambda v: -sum(min(a, RING - a) for a in v))
LOW = -3.0e38
CHUNK = 256
EARLY = 3
GROUPS = ((0,), (1,), (2,), (3,), (4,), (5,), (6,), (7,))
MESH = pl.DeviceIdType.MESH


def kernel(qh, dh, nh, qm, dm, nm, te, w, tau_ref, loss_ref, mean_ref,
           qv, dv, nv, qmv, dmv, nmv, tev, wv, gath, docs, negs, best, hard, ones, dense, rest_ref, inbox,
           in_sem, doc_sem, gsend, grecv, osend, orecv):
    me = lax.axis_index('data')
    core = lax.rem(me, 2)
    chip = me // 2
    pos = (lax.rem(chip, RING), lax.rem(chip // RING, RING), chip // (RING * RING))
    nq, dlen, width = dv.shape
    nneg, qlen, proj = nv.shape[1], qv.shape[1], wv.shape[1]
    tau = tau_ref[0]

    def device(steps, other=0):
        c = [lax.rem(pos[a] + steps[a], RING) if steps[a] else pos[a] for a in range(3)]
        return {'data': ((c[2] * RING + c[1]) * RING + c[0]) * 2 + (1 - core if other else core)}

    def along(axis, off):
        return device([off if a == axis else 0 for a in range(3)])

    partner = device((0, 0, 0), 1)

    def remote(src, dst, send, recv, target):
        return pltpu.make_async_remote_copy(src_ref=src, dst_ref=dst, send_sem=send, recv_sem=recv,
                                            device_id=target, device_id_type=MESH)

    pairs = ((w, wv), (qh, qv), (qm, qmv), (dm, dmv), (nm, nmv), (te, tev))
    loads = [pltpu.make_async_copy(src, dst, in_sem.at[n]) for n, (src, dst) in enumerate(pairs)]
    first, small = loads[:3], loads[3:]
    doc_load = pltpu.make_async_copy(dh, dv, in_sem.at[6])
    neg_loads = [pltpu.make_async_copy(nh.at[i], nv.at[i], in_sem.at[7 + i]) for i in range(nq)]
    for load in first + small + [doc_load] + neg_loads:
        load.start()

    barrier = pltpu.get_barrier_semaphore()
    for axis in range(3):
        for off in range(1, RING):
            pl.semaphore_signal(barrier, inc=1, device_id=along(axis, off), device_id_type=MESH)
    pl.semaphore_signal(barrier, inc=1, device_id=partner, device_id_type=MESH)

    def project(rows):
        y = jnp.dot(rows, wv[...], preferred_element_type=jnp.float32)
        return y * lax.rsqrt(jnp.sum(y * y, axis=-1, keepdims=True))

    def length(mask_row):
        return jnp.sum(mask_row.astype(jnp.float32), axis=-1, keepdims=True)

    def row_ids(rows, cols):
        return lax.broadcasted_iota(jnp.int32, (rows, cols), 0).astype(jnp.float32)

    hard[...] = jnp.zeros_like(hard)
    dense[...] = jnp.zeros_like(dense)
    e_row = lax.broadcasted_iota(jnp.int32, ones.shape, 0)
    e_lane = lax.rem(lax.broadcasted_iota(jnp.int32, ones.shape, 1), RING) * qlen
    ones[...] = jnp.where((e_row >= e_lane) & (e_row < e_lane + qlen), 1.0, 0.0)

    for load in first:
        load.wait()
    for q in range(nq):
        tok = project(qv[q])
        keep = row_ids(qlen, proj) < length(qmv[q:q + 1, :])
        gath[q * RING + pos[ORDERS[q][0]]] = jnp.where(keep, tok, 0.0).astype(jnp.bfloat16)

    pl.semaphore_wait(barrier, 3 * (RING - 1) + 1)

    slot_of = {pair: n for n, pair in enumerate(SLOTS)}

    for off in NEAR_FIRST:
        for q in range(nq):
            a1 = ORDERS[q][0]
            block = gath.at[q * RING + pos[a1]]
            remote(block, block, gsend, grecv.at[0], along(a1, off)).start()

    def row_of(n, q):
        return gath.at[pl.ds((n * nq + q) * RING, RING)]

    def send_row(r, level):
        for off in NEAR_FIRST:
            back = (0, RING - off) if level == 1 else (RING - off, r)
            for q in range(nq):
                n = slot_of[back]
                remote(row_of(slot_of[(0, r)], q), row_of(n, q), gsend, grecv.at[n],
                       along(ORDERS[q][level], off)).start()

    def arrived(n):
        part = gath.at[pl.ds(n * nq * RING, nq * RING if n else nq * (RING - 1))]
        remote(part, part, gsend, grecv.at[n], partner).wait_recv()

    for load in small + [doc_load]:
        load.wait()

    def document(rows, mask_row, out):
        limit = length(mask_row)
        head = None
        for c in range(dlen // CHUNK):
            part = pl.ds(c * CHUNK, CHUNK)
            y = project(rows[part, :])
            head = y[0:1, :] if head is None else head
            out[part, :] = jnp.where(row_ids(CHUNK, proj) + c * CHUNK < limit, y, head).astype(jnp.bfloat16)

    for j in range(nq):
        document(dv.at[j], dmv[j:j + 1, :], docs.at[core * nq + j])

    my_docs = docs.at[pl.ds(core * nq, nq)]
    their_docs = docs.at[pl.ds((1 - core) * nq, nq)]
    doc_send = remote(my_docs, my_docs, doc_sem.at[0], doc_sem.at[1], partner)
    doc_recv = remote(their_docs, their_docs, doc_sem.at[0], doc_sem.at[1], partner)
    contract = (((1,), (1,)), ((), ()))
    cell_row = lax.broadcasted_iota(jnp.int32, (8, proj), 0)
    cell_lane = lax.broadcasted_iota(jnp.int32, (8, proj), 1)
    cell = cell_row * (proj // RING) + cell_lane // RING

    def negative(i, k):
        if k == 0:
            neg_loads[i].wait()
        document(nv.at[i, k], nmv[i, k:k + 1, :], negs.at[i * nneg + k])

    def hard_scores():
        found = hard[...]
        for i in range(nq):
            mine = gath[i * RING + pos[ORDERS[i][0]]]
            for k in range(nneg):
                sim = lax.dot_general(negs[i * nneg + k], mine, contract, preferred_element_type=jnp.float32)
                score = jnp.sum(jnp.max(sim, axis=0, keepdims=True), axis=1, keepdims=True)
                found = jnp.where((cell_row == i) & (cell_lane == k + 1), score, found)
        hard[...] = found

    def place(q, i3, i2):
        a1, a2, a3 = ORDERS[q]
        return (q * RING + lax.rem(pos[a3] + i3, RING)) * RING + lax.rem(pos[a2] + i2, RING)

    pieces = 2 * nq
    tile = 2 * proj
    tile_row = lax.broadcasted_iota(jnp.int32, (8, tile), 0)

    def segment(s, tiles):
        for t in tiles:
            at = s * pieces * RING + 2 * t * RING
            rows = gath[at:at + 2 * RING].reshape(tile, proj)
            unit = jnp.zeros((8, tile), jnp.float32)
            for j in range(2 * nq):
                sim = lax.dot_general(docs[j], rows, contract,
                                      preferred_element_type=jnp.float32)
                unit = jnp.where(tile_row == j, jnp.max(sim, axis=0, keepdims=True), unit)
            best[s % 2, 2 * t] = unit[:, :proj]
            best[s % 2, 2 * t + 1] = unit[:, proj:]

    def reduce_segment(s):
        flat = best[s % 2].reshape(pieces * 8, proj)
        scores = lax.dot_general(flat, ones[...], (((1,), (0,)), ((), ())), precision=lax.Precision.HIGHEST,
                                 preferred_element_type=jnp.float32).reshape(pieces, 8, proj)
        real = lax.broadcasted_iota(jnp.int32, scores.shape, 1) < 2 * nq
        top = jnp.max(jnp.where(real, scores, LOW), axis=1, keepdims=True)
        mass = jnp.sum(jnp.where(real, jnp.exp((scores - top) / tau), 0.0), axis=1, keepdims=True)
        part = top / tau + jnp.log(mass)
        packed = dense[...]
        for p in range(pieces):
            i3, i2 = SLOTS[2 * s + p // nq]
            packed = jnp.where(cell == place(p % nq, i3, i2), part[p], packed)
        dense[...] = packed
        if s == 0:
            students = hard[...]
            for q in range(nq):
                here = (cell_row == core * nq + q) & (cell_lane == pos[ORDERS[q][0]])
                hit = jnp.sum(jnp.where(here, scores[q], 0.0), axis=0, keepdims=True)
                hit = jnp.sum(hit, axis=1, keepdims=True)
                students = jnp.where((cell_row == q) & (cell_lane == 0), hit, students)
            hard[...] = students

    def log_softmax(z):
        z = z - jnp.max(z, axis=1, keepdims=True)
        return z - jnp.log(jnp.sum(jnp.exp(z), axis=1, keepdims=True))

    def finish_rows():
        logits = hard[:nq, :nneg + 1] / tau
        teacher_log = log_softmax(tev[...])
        student_log = log_softmax(logits)
        rest = jnp.sum(jnp.exp(teacher_log) * (teacher_log - student_log), axis=1, keepdims=True) - logits[:, 0:1]
        rest_ref[...] = jnp.broadcast_to(rest, rest_ref.shape)
        rest_sum = jnp.sum(rest, axis=0, keepdims=True)
        dense[...] = jnp.where((cell_row == 1) & (cell_lane == proj - 1), rest_sum, dense[...])

    negative(0, 0)
    doc_send.start()
    for n in range(1, EARLY):
        negative(n // nneg, n % nneg)
    arrived(0)
    send_row(0, 1)
    send_row(0, 2)
    for n in range(EARLY, nq * nneg):
        negative(n // nneg, n % nneg)
    hard_scores()
    doc_recv.wait_recv()
    segment(0, (0,))
    for group in GROUPS:
        for n in range(2 * group[0], 2 * group[-1] + 2):
            if SLOTS[n][0]:
                arrived(n)
            elif n:
                arrived(n)
                send_row(SLOTS[n][1], 2)
        for s in group:
            if s:
                reduce_segment(s - 1)
            if s == 2:
                finish_rows()
            segment(s, (0, 1, 2) if s else (1, 2))
    reduce_segment(len(SLOTS) // 2 - 1)

    here = core * CHIPS + chip
    inbox[here] = dense[0:2, :]
    mine = inbox.at[here]
    for steps in OTHERS + [(0, 0, 0)]:
        for other in (0, 1):
            if other or any(steps):
                remote(mine, mine, osend, orecv, device(steps, other)).start()
    others = inbox.at[pl.ds(0, 2 * CHIPS - 1)]
    remote(others, others, osend, orecv, partner).wait_recv()

    r_id = lax.broadcasted_iota(jnp.int32, (2, proj), 0)
    l_id = lax.broadcasted_iota(jnp.int32, (2, proj), 1)
    r_cell = r_id * (proj // RING) + l_id // RING

    def merged(which):
        parts = inbox[pl.ds(which * CHIPS, CHIPS)]
        top = jnp.max(parts, axis=0)
        lse = top + jnp.log(jnp.sum(jnp.exp(parts - top[None]), axis=0))
        extra = jnp.where((r_id == 1) & (l_id == proj - 1), jnp.sum(parts, axis=0), 0.0)
        return lse, jnp.where(r_cell < nq * RING * RING, lse, extra)

    lse, total = merged(core)
    total = total + merged(1 - core)[1]
    mean_ref[0] = jnp.sum(total) / (2 * CHIPS * nq)
    for q in range(nq):
        spot = (r_cell == place(q, 0, 0)) & (lax.rem(l_id, RING) == pos[ORDERS[q][0]])
        loss_ref[q] = jnp.sum(jnp.where(spot, lse, 0.0) + jnp.where((r_id == 0) & (l_id == 0), rest_ref[q:q + 1, :], 0.0))

    doc_send.wait_send()
    remote(others, others, osend, orecv, partner).wait_send()
    sent = gath.at[pl.ds(0, nq * (RING - 1) + (len(SLOTS) - 1) * nq * RING)]
    remote(sent, sent, gsend, grecv.at[0], partner).wait_send()


def solution(mesh):
    batch_axes = ('replica', 'data')

    def local_loss(query_hidden, doc_hidden, neg_hidden, query_mask, doc_mask, neg_mask, teacher, w_proj, temperature):
        nq, qlen, width = query_hidden.shape
        dlen, nneg = doc_hidden.shape[1], neg_hidden.shape[1]
        proj = w_proj.shape[1]
        anywhere = pl.BlockSpec(memory_space=pl.ANY)
        smem = pl.BlockSpec(memory_space=pltpu.SMEM)
        rows = nq * (qlen + dlen + nneg * dlen)
        loss, mean = pl.pallas_call(
            kernel,
            name='late_interaction',
            out_shape=(jax.ShapeDtypeStruct((nq,), jnp.float32), jax.ShapeDtypeStruct((1,), jnp.float32)),
            in_specs=[anywhere] * 8 + [smem],
            out_specs=(smem, smem),
            scratch_shapes=[
                pltpu.VMEM(query_hidden.shape, jnp.bfloat16),
                pltpu.VMEM(doc_hidden.shape, jnp.bfloat16),
                pltpu.VMEM(neg_hidden.shape, jnp.bfloat16),
                pltpu.VMEM(query_mask.shape, jnp.int32),
                pltpu.VMEM(doc_mask.shape, jnp.int32),
                pltpu.VMEM(neg_mask.shape, jnp.int32),
                pltpu.VMEM(teacher.shape, jnp.float32),
                pltpu.VMEM(w_proj.shape, jnp.bfloat16),
                pltpu.VMEM((len(SLOTS) * nq * RING, qlen, proj), jnp.bfloat16),
                pltpu.VMEM((2 * nq, dlen, proj), jnp.bfloat16),
                pltpu.VMEM((nq * nneg, dlen, proj), jnp.bfloat16),
                pltpu.VMEM((2, 2 * nq, 8, proj), jnp.float32),
                pltpu.VMEM((8, proj), jnp.float32),
                pltpu.VMEM((proj, proj), jnp.float32),
                pltpu.VMEM((8, proj), jnp.float32),
                pltpu.VMEM((nq, proj), jnp.float32),
                pltpu.VMEM((2 * CHIPS, 2, proj), jnp.float32),
                pltpu.SemaphoreType.DMA((7 + nq,)),
                pltpu.SemaphoreType.DMA((2,)),
                pltpu.SemaphoreType.DMA,
                pltpu.SemaphoreType.DMA((len(SLOTS),)),
                pltpu.SemaphoreType.DMA,
                pltpu.SemaphoreType.DMA,
            ],
            compiler_params=pltpu.CompilerParams(
                collective_id=0, has_side_effects=True, vmem_limit_bytes=60 * 1024 * 1024),
            cost_estimate=pl.CostEstimate(
                flops=2 * proj * (rows * width + CHIPS * nq * qlen * 2 * nq * dlen),
                bytes_accessed=2 * rows * width, transcendentals=rows),
        )(query_hidden, doc_hidden, neg_hidden, query_mask, doc_mask, neg_mask, teacher, w_proj,
          temperature.reshape(1))
        return loss, mean

    in_specs = (P(batch_axes, None, None), P(batch_axes, None, None), P(batch_axes, None, None, None),
                P(batch_axes, None), P(batch_axes, None), P(batch_axes, None, None), P(batch_axes, None),
                P(None, None), P())
    out_specs = (P(batch_axes), P('replica'))
    return jax.shard_map(local_loss, mesh=mesh, in_specs=in_specs, out_specs=out_specs, check_vma=False)
```

```python
import jax
import jax.numpy as jnp
from jax import lax
from jax.experimental import pallas as pl
from jax.experimental.pallas import tpu as pltpu
from jax.sharding import PartitionSpec as P

RING = 4
CHIPS = RING ** 3
ORDERS = ((0, 1, 2), (1, 2, 0), (2, 0, 1))
NEAR_FIRST = (1, 3, 2)
STEPS = range(1, RING)
QUERIES = range(len(ORDERS))


def layout():
    runs, blocks = {}, []

    def add(name, members):
        runs[name] = (len(blocks), len(members))
        blocks.extend(members)

    add('cross', [b for q in QUERIES for b in
                  [(q, 0, 0, 0)] + [(q, 0, 0, c) for c in STEPS] + [(q, 0, r, 0) for r in STEPS]
                  + [(q, p, 0, 0) for p in STEPS]])
    for r in NEAR_FIRST:
        add((0, r), [(q, 0, r, c) for q in QUERIES for c in STEPS])
    for p in NEAR_FIRST:
        add((p, 0), [b for q in QUERIES for b in
                     [(q, p, 0, c) for c in STEPS] + [(q, p, r, 0) for r in STEPS]])
    for p, r in ((1, 1), (3, 1), (1, 3), (3, 3), (2, 1), (2, 3), (1, 2), (3, 2), (2, 2)):
        add((p, r), [(q, p, r, c) for q in QUERIES for c in STEPS])
    return runs, blocks


RUNS, BLOCKS = layout()
CROSS = len(BLOCKS[:RUNS['cross'][1]]) // len(ORDERS)
TILE = 8
GROUPS = ((0, 1, 2), (3, 4, 5, 6), (7, 8, 9), (10, 11, 12), (13, 14, 15), (16, 17, 18, 19), (20, 21, 22, 23))
OTHERS = sorted([(x, y, z) for x in range(RING) for y in range(RING) for z in range(RING) if x or y or z],
                key=lambda v: -sum(min(a, RING - a) for a in v))
LOW = -3.0e38
CHUNK = 256
EARLY = 8
MESH = pl.DeviceIdType.MESH


def kernel(qh, dh, nh, qm, dm, nm, te, w, tau_ref, out_ref,
           qv, dv, nv, qmv, dmv, nmv, tev, wv, gath, docs, negs, best, hard, ones, dense, rest_ref, inbox,
           in_sem, doc_sem, gsend, grecv, osend, orecv):
    me = lax.axis_index('data')
    core = lax.rem(me, 2)
    chip = me // 2
    pos = (lax.rem(chip, RING), lax.rem(chip // RING, RING), chip // (RING * RING))
    nq, dlen, width = dv.shape
    nneg, qlen, proj = nv.shape[1], qv.shape[1], wv.shape[1]
    tau = tau_ref[0]

    def device(steps, other=0):
        c = [lax.rem(pos[a] + steps[a], RING) if steps[a] else pos[a] for a in range(3)]
        return {'data': ((c[2] * RING + c[1]) * RING + c[0]) * 2 + (1 - core if other else core)}

    def along(axis, off):
        return device([off if a == axis else 0 for a in range(3)])

    partner = device((0, 0, 0), 1)

    def remote(src, dst, send, recv, target):
        return pltpu.make_async_remote_copy(src_ref=src, dst_ref=dst, send_sem=send, recv_sem=recv,
                                            device_id=target, device_id_type=MESH)

    pairs = ((w, wv), (qh, qv), (qm, qmv), (dm, dmv), (nm, nmv), (te, tev))
    loads = [pltpu.make_async_copy(src, dst, in_sem.at[n]) for n, (src, dst) in enumerate(pairs)]
    first, small = loads[:3], loads[3:]
    doc_load = pltpu.make_async_copy(dh, dv, in_sem.at[6])
    neg_loads = [pltpu.make_async_copy(nh.at[i], nv.at[i], in_sem.at[7 + i]) for i in range(nq)]
    for load in first + small + [doc_load] + neg_loads:
        load.start()

    barrier = pltpu.get_barrier_semaphore()
    for axis in range(3):
        for off in range(1, RING):
            pl.semaphore_signal(barrier, inc=1, device_id=along(axis, off), device_id_type=MESH)
    pl.semaphore_signal(barrier, inc=1, device_id=partner, device_id_type=MESH)

    def project(rows):
        y = jnp.dot(rows, wv[...], preferred_element_type=jnp.float32)
        return y * lax.rsqrt(jnp.sum(y * y, axis=-1, keepdims=True))

    def length(mask_row):
        return jnp.sum(mask_row.astype(jnp.float32), axis=-1, keepdims=True)

    def row_ids(rows, cols):
        return lax.broadcasted_iota(jnp.int32, (rows, cols), 0).astype(jnp.float32)

    hard[...] = jnp.zeros_like(hard)
    dense[...] = jnp.zeros_like(dense)
    e_row = lax.broadcasted_iota(jnp.int32, ones.shape, 0)
    e_from = lax.broadcasted_iota(jnp.int32, ones.shape, 1) // proj * qlen
    ones[...] = jnp.where((e_row >= e_from) & (e_row < e_from + qlen), 1.0, 0.0).astype(jnp.bfloat16)

    for load in first:
        load.wait()
    for q in range(nq):
        tok = project(qv[q])
        keep = row_ids(qlen, proj) < length(qmv[q:q + 1, :])
        gath[q * CROSS] = jnp.where(keep, tok, 0.0).astype(jnp.bfloat16)

    pl.semaphore_wait(barrier, 3 * (RING - 1) + 1)

    sems = {name: n for n, name in enumerate(RUNS)}

    def send(first, count, name, place_at, axis, off):
        at = RUNS[name][0] + place_at
        remote(gath.at[pl.ds(first, count)], gath.at[pl.ds(at, count)], gsend, grecv.at[sems[name]],
               along(axis, off)).start()

    def arrived(name):
        at, count = RUNS[name]
        part = gath.at[pl.ds(at, count if name != 'cross' else count - nq)]
        remote(part, part, gsend, grecv.at[sems[name]], partner).wait_recv()

    for off in NEAR_FIRST:
        for q in range(nq):
            for level in range(3):
                send(q * CROSS, 1, 'cross', q * CROSS + level * (RING - 1) + RING - off, ORDERS[q][level], off)

    def send_cross():
        for off in NEAR_FIRST:
            for q in range(nq):
                send(q * CROSS + 1, 3, (0, RING - off), 3 * q, ORDERS[q][1], off)
        for off in NEAR_FIRST:
            for q in range(nq):
                send(q * CROSS + 1, 6, (RING - off, 0), 6 * q, ORDERS[q][2], off)

    def send_row(r):
        for off in NEAR_FIRST:
            for q in range(nq):
                send(RUNS[(0, r)][0] + 3 * q, 3, (RING - off, r), 3 * q, ORDERS[q][2], off)

    for load in small + [doc_load]:
        load.wait()

    def document(rows, mask_row, out):
        limit = length(mask_row)
        head = None
        for c in range(dlen // CHUNK):
            part = pl.ds(c * CHUNK, CHUNK)
            y = project(rows[part, :])
            head = y[0:1, :] if head is None else head
            out[part, :] = jnp.where(row_ids(CHUNK, proj) + c * CHUNK < limit, y, head).astype(jnp.bfloat16)

    for j in range(nq):
        document(dv.at[j], dmv[j:j + 1, :], docs.at[core * nq + j])

    my_docs = docs.at[pl.ds(core * nq, nq)]
    their_docs = docs.at[pl.ds((1 - core) * nq, nq)]
    doc_send = remote(my_docs, my_docs, doc_sem.at[0], doc_sem.at[1], partner)
    doc_recv = remote(their_docs, their_docs, doc_sem.at[0], doc_sem.at[1], partner)
    contract = (((1,), (1,)), ((), ()))
    cell_row = lax.broadcasted_iota(jnp.int32, (8, proj), 0)
    cell_lane = lax.broadcasted_iota(jnp.int32, (8, proj), 1)
    cell = cell_row * proj + cell_lane

    def negative(i, k):
        if k == 0:
            neg_loads[i].wait()
        document(nv.at[i, k], nmv[i, k:k + 1, :], negs.at[i * nneg + k])

    def hard_scores():
        found = hard[...]
        for i in range(nq):
            mine = gath[i * CROSS]
            for k in range(nneg):
                sim = lax.dot_general(negs[i * nneg + k], mine, contract, preferred_element_type=jnp.float32)
                score = jnp.sum(jnp.max(sim, axis=0, keepdims=True), axis=1, keepdims=True)
                found = jnp.where((cell_row == i) & (cell_lane == k + 1), score, found)
        hard[...] = found

    def place(q, p, r, c):
        index = q
        for axis, steps in zip(reversed(ORDERS[q]), (p, r, c)):
            index = index * RING + (lax.rem(pos[axis] + steps, RING) if steps else pos[axis])
        return index

    tile = TILE * qlen
    tile_row = lax.broadcasted_iota(jnp.int32, (8, tile), 0)

    def segment(g):
        for n, t in enumerate(GROUPS[g]):
            rows = gath[t * TILE:(t + 1) * TILE].reshape(tile, proj)
            unit = jnp.zeros((8, tile), jnp.float32)
            for j in range(2 * nq):
                sim = lax.dot_general(docs[j], rows, contract, preferred_element_type=jnp.float32)
                unit = jnp.where(tile_row == j, jnp.max(sim, axis=0, keepdims=True), unit)
            best[g % 2, 2 * n] = unit[:, :proj]
            best[g % 2, 2 * n + 1] = unit[:, proj:]

    def reduce_segment(g):
        pieces = 2 * len(GROUPS[g])
        per = proj // qlen
        flat = best[g % 2, :pieces].reshape(pieces * 8, proj)
        high = flat.astype(jnp.bfloat16)
        left = flat - high.astype(jnp.float32)
        middle = left.astype(jnp.bfloat16)
        low = (left - middle.astype(jnp.float32)).astype(jnp.bfloat16)
        sums = jnp.dot(jnp.concatenate([high, middle, low], axis=0), ones[...], preferred_element_type=jnp.float32)
        size = pieces * 8
        scores = (sums[:size] + sums[size:2 * size] + sums[2 * size:]).reshape(pieces, 8, per * proj)
        real = lax.broadcasted_iota(jnp.int32, scores.shape, 1) < 2 * nq
        top = jnp.max(jnp.where(real, scores, LOW), axis=1, keepdims=True)
        mass = jnp.sum(jnp.where(real, jnp.exp((scores - top) / tau), 0.0), axis=1, keepdims=True)
        part = top / tau + jnp.log(mass)
        packed = dense[...]
        first = GROUPS[g][0] * TILE
        for b in range(pieces * per):
            values = lax.slice(part, (b // per, 0, b % per * proj), (b // per + 1, 1, (b % per + 1) * proj))[0]
            packed = jnp.where(cell == place(*BLOCKS[first + b]), values, packed)
        dense[...] = packed
        if g == 0:
            students = hard[...]
            for q in range(nq):
                b = q * CROSS
                column = lax.slice(scores, (b // per, 0, b % per * proj), (b // per + 1, 8, (b % per + 1) * proj))[0]
                hit = jnp.sum(jnp.where(cell_row == core * nq + q, column, 0.0), axis=0, keepdims=True)
                students = jnp.where((cell_row == q) & (cell_lane == 0), hit, students)
            hard[...] = students

    def log_softmax(z):
        z = z - jnp.max(z, axis=1, keepdims=True)
        return z - jnp.log(jnp.sum(jnp.exp(z), axis=1, keepdims=True))

    def finish_rows():
        logits = hard[:nq, :nneg + 1] / tau
        teacher_log = log_softmax(tev[...])
        student_log = log_softmax(logits)
        rest = jnp.sum(jnp.exp(teacher_log) * (teacher_log - student_log), axis=1, keepdims=True) - logits[:, 0:1]
        rest_ref[...] = jnp.broadcast_to(rest, rest_ref.shape)
        rest_sum = jnp.sum(rest, axis=0, keepdims=True)
        dense[...] = jnp.where((cell_row == 1) & (cell_lane == proj - 1), rest_sum, dense[...])

    negative(0, 0)
    doc_send.start()
    for n in range(1, EARLY):
        negative(n // nneg, n % nneg)
    arrived('cross')
    send_cross()
    for n in range(EARLY, nq * nneg):
        negative(n // nneg, n % nneg)
    hard_scores()
    doc_recv.wait_recv()
    waited = {'cross'}
    for g, group in enumerate(GROUPS):
        for name, (at, count) in RUNS.items():
            if at < (group[-1] + 1) * TILE and name not in waited:
                waited.add(name)
                arrived(name)
                if not name[0]:
                    send_row(name[1])
        if g:
            reduce_segment(g - 1)
        if g == 2:
            finish_rows()
        segment(g)
    reduce_segment(len(GROUPS) - 1)

    here = core * CHIPS + chip
    inbox[here] = dense[0:2, :]
    mine = inbox.at[here]
    for steps in OTHERS + [(0, 0, 0)]:
        for other in (0, 1):
            if other or any(steps):
                remote(mine, mine, osend, orecv, device(steps, other)).start()
    others = inbox.at[pl.ds(0, 2 * CHIPS - 1)]
    remote(others, others, osend, orecv, partner).wait_recv()

    r_id = lax.broadcasted_iota(jnp.int32, (2, proj), 0)
    l_id = lax.broadcasted_iota(jnp.int32, (2, proj), 1)
    r_cell = r_id * proj + l_id

    def merged(which):
        parts = inbox[pl.ds(which * CHIPS, CHIPS)]
        top = jnp.max(parts, axis=0)
        lse = top + jnp.log(jnp.sum(jnp.exp(parts - top[None]), axis=0))
        extra = jnp.where((r_id == 1) & (l_id == proj - 1), jnp.sum(parts, axis=0), 0.0)
        return lse, jnp.where(r_cell < nq * CHIPS, lse, extra)

    lse, total = merged(core)
    total = total + merged(1 - core)[1]
    out_ref[nq] = jnp.sum(total) / (2 * CHIPS * nq)
    for q in range(nq):
        spot = r_cell == place(q, 0, 0, 0)
        out_ref[q] = jnp.sum(jnp.where(spot, lse, 0.0) + jnp.where((r_id == 0) & (l_id == 0), rest_ref[q:q + 1, :], 0.0))

    doc_send.wait_send()
    remote(others, others, osend, orecv, partner).wait_send()
    sent = gath.at[pl.ds(0, len(BLOCKS) - nq)]
    remote(sent, sent, gsend, grecv.at[0], partner).wait_send()


def solution(mesh):
    batch_axes = ('replica', 'data')

    def local_loss(query_hidden, doc_hidden, neg_hidden, query_mask, doc_mask, neg_mask, teacher, w_proj, temperature):
        nq, qlen, width = query_hidden.shape
        dlen, nneg = doc_hidden.shape[1], neg_hidden.shape[1]
        proj = w_proj.shape[1]
        anywhere = pl.BlockSpec(memory_space=pl.ANY)
        smem = pl.BlockSpec(memory_space=pltpu.SMEM)
        rows = nq * (qlen + dlen + nneg * dlen)
        result = pl.pallas_call(
            kernel,
            name='late_interaction',
            out_shape=jax.ShapeDtypeStruct((nq + 1,), jnp.float32),
            in_specs=[anywhere] * 8 + [smem],
            out_specs=smem,
            scratch_shapes=[
                pltpu.VMEM(query_hidden.shape, jnp.bfloat16),
                pltpu.VMEM(doc_hidden.shape, jnp.bfloat16),
                pltpu.VMEM(neg_hidden.shape, jnp.bfloat16),
                pltpu.VMEM(query_mask.shape, jnp.int32),
                pltpu.VMEM(doc_mask.shape, jnp.int32),
                pltpu.VMEM(neg_mask.shape, jnp.int32),
                pltpu.VMEM(teacher.shape, jnp.float32),
                pltpu.VMEM(w_proj.shape, jnp.bfloat16),
                pltpu.VMEM((len(BLOCKS), qlen, proj), jnp.bfloat16),
                pltpu.VMEM((2 * nq, dlen, proj), jnp.bfloat16),
                pltpu.VMEM((nq * nneg, dlen, proj), jnp.bfloat16),
                pltpu.VMEM((2, 2 * max(map(len, GROUPS)), 8, proj), jnp.float32),
                pltpu.VMEM((8, proj), jnp.float32),
                pltpu.VMEM((proj, proj // qlen * proj), jnp.bfloat16),
                pltpu.VMEM((8, proj), jnp.float32),
                pltpu.VMEM((nq, proj), jnp.float32),
                pltpu.VMEM((2 * CHIPS, 2, proj), jnp.float32),
                pltpu.SemaphoreType.DMA((7 + nq,)),
                pltpu.SemaphoreType.DMA((2,)),
                pltpu.SemaphoreType.DMA,
                pltpu.SemaphoreType.DMA((len(RUNS),)),
                pltpu.SemaphoreType.DMA,
                pltpu.SemaphoreType.DMA,
            ],
            compiler_params=pltpu.CompilerParams(
                collective_id=0, has_side_effects=True, vmem_limit_bytes=60 * 1024 * 1024),
            cost_estimate=pl.CostEstimate(
                flops=2 * proj * (rows * width + CHIPS * nq * qlen * 2 * nq * dlen),
                bytes_accessed=2 * rows * width, transcendentals=rows),
        )(query_hidden, doc_hidden, neg_hidden, query_mask, doc_mask, neg_mask, teacher, w_proj,
          temperature.reshape(1))
        return result[:nq], result[nq:]

    in_specs = (P(batch_axes, None, None), P(batch_axes, None, None), P(batch_axes, None, None, None),
                P(batch_axes, None), P(batch_axes, None), P(batch_axes, None, None), P(batch_axes, None),
                P(None, None), P())
    out_specs = (P(batch_axes), P('replica'))
    return jax.shard_map(local_loss, mesh=mesh, in_specs=in_specs, out_specs=out_specs, check_vma=False)
```

```python
import jax
import jax.numpy as jnp
from jax import lax
from jax.experimental import pallas as pl
from jax.experimental.pallas import tpu as pltpu
from jax.sharding import PartitionSpec as P

RING = 4
CHIPS = RING ** 3
ORDERS = ((0, 1, 2), (1, 2, 0), (2, 0, 1))
NEAR_FIRST = (1, 3, 2)
STEPS = range(1, RING)
QUERIES = range(len(ORDERS))


def layout():
    runs, blocks = {}, []

    def add(name, members):
        runs[name] = (len(blocks), len(members))
        blocks.extend(members)

    add('cross', [b for q in QUERIES for b in
                  [(q, 0, 0, 0)] + [(q, 0, 0, c) for c in STEPS] + [(q, 0, r, 0) for r in STEPS]
                  + [(q, p, 0, 0) for p in STEPS]])
    for r in NEAR_FIRST:
        add((0, r), [(q, 0, r, c) for q in QUERIES for c in STEPS])
    for p in NEAR_FIRST:
        add((p, 0), [b for q in QUERIES for b in
                     [(q, p, 0, c) for c in STEPS] + [(q, p, r, 0) for r in STEPS]])
    for p, r in ((1, 1), (3, 1), (1, 3), (3, 3), (2, 1), (2, 3), (1, 2), (3, 2), (2, 2)):
        add((p, r), [(q, p, r, c) for q in QUERIES for c in STEPS])
    return runs, blocks


RUNS, BLOCKS = layout()
CROSS = len(BLOCKS[:RUNS['cross'][1]]) // len(ORDERS)
TILE = 8
GROUPS = ((0, 1, 2), (3, 4, 5, 6), (7, 8, 9), (10, 11, 12), (13, 14, 15), (16, 17, 18, 19), (20, 21, 22, 23))
OTHERS = sorted([(x, y, z) for x in range(RING) for y in range(RING) for z in range(RING) if x or y or z],
                key=lambda v: -sum(min(a, RING - a) for a in v))
LOW = -3.0e38
CHUNK = 256
EARLY = 8
MESH = pl.DeviceIdType.MESH


def kernel(qh, dh, nh, qm, dm, nm, te, w, tau_ref, out_ref,
           qv, dv, nv, qmv, dmv, nmv, tev, wv, gath, docs, negs, best, hard, ones, dense, rest_ref, inbox,
           in_sem, doc_sem, gsend, grecv, osend, orecv):
    me = lax.axis_index('data')
    core = lax.rem(me, 2)
    chip = me // 2
    pos = (lax.rem(chip, RING), lax.rem(chip // RING, RING), chip // (RING * RING))
    nq, dlen, width = dv.shape
    nneg, qlen, proj = nv.shape[1], qv.shape[1], wv.shape[1]
    tau = tau_ref[0]

    def device(steps, other=0):
        c = [lax.rem(pos[a] + steps[a], RING) if steps[a] else pos[a] for a in range(3)]
        return {'data': ((c[2] * RING + c[1]) * RING + c[0]) * 2 + (1 - core if other else core)}

    def along(axis, off):
        return device([off if a == axis else 0 for a in range(3)])

    partner = device((0, 0, 0), 1)

    def remote(src, dst, send, recv, target):
        return pltpu.make_async_remote_copy(src_ref=src, dst_ref=dst, send_sem=send, recv_sem=recv,
                                            device_id=target, device_id_type=MESH)

    pairs = ((w, wv), (qh, qv), (qm, qmv), (dm, dmv), (nm, nmv), (te, tev))
    loads = [pltpu.make_async_copy(src, dst, in_sem.at[n]) for n, (src, dst) in enumerate(pairs)]
    first, small = loads[:3], loads[3:]
    doc_load = pltpu.make_async_copy(dh, dv, in_sem.at[6])
    neg_loads = [pltpu.make_async_copy(nh.at[i], nv.at[i], in_sem.at[7 + i]) for i in range(nq)]
    for load in first + small + [doc_load] + neg_loads:
        load.start()

    barrier = pltpu.get_barrier_semaphore()
    for axis in range(3):
        for off in range(1, RING):
            pl.semaphore_signal(barrier, inc=1, device_id=along(axis, off), device_id_type=MESH)
    pl.semaphore_signal(barrier, inc=1, device_id=partner, device_id_type=MESH)

    def project(rows):
        y = jnp.dot(rows, wv[...], preferred_element_type=jnp.float32)
        return y * lax.rsqrt(jnp.sum(y * y, axis=-1, keepdims=True))

    def length(mask_row):
        return jnp.sum(mask_row.astype(jnp.float32), axis=-1, keepdims=True)

    def row_ids(rows, cols):
        return lax.broadcasted_iota(jnp.int32, (rows, cols), 0).astype(jnp.float32)

    hard[...] = jnp.zeros_like(hard)
    dense[...] = jnp.zeros_like(dense)
    e_row = lax.broadcasted_iota(jnp.int32, ones.shape, 0)
    e_from = lax.broadcasted_iota(jnp.int32, ones.shape, 1) // proj * qlen
    ones[...] = jnp.where((e_row >= e_from) & (e_row < e_from + qlen), 1.0, 0.0).astype(jnp.bfloat16)

    for load in first:
        load.wait()
    for q in range(nq):
        tok = project(qv[q])
        keep = row_ids(qlen, proj) < length(qmv[q:q + 1, :])
        gath[q * CROSS] = jnp.where(keep, tok, 0.0).astype(jnp.bfloat16)

    pl.semaphore_wait(barrier, 3 * (RING - 1) + 1)

    sems = {name: n for n, name in enumerate(RUNS)}

    def send(first, count, name, place_at, axis, off):
        at = RUNS[name][0] + place_at
        remote(gath.at[pl.ds(first, count)], gath.at[pl.ds(at, count)], gsend, grecv.at[sems[name]],
               along(axis, off)).start()

    def arrived(name):
        at, count = RUNS[name]
        part = gath.at[pl.ds(at, count if name != 'cross' else count - nq)]
        remote(part, part, gsend, grecv.at[sems[name]], partner).wait_recv()

    for off in NEAR_FIRST:
        for q in range(nq):
            for level in range(3):
                send(q * CROSS, 1, 'cross', q * CROSS + level * (RING - 1) + RING - off, ORDERS[q][level], off)

    def send_cross():
        for off in NEAR_FIRST:
            for q in range(nq):
                send(q * CROSS + 1, 3, (0, RING - off), 3 * q, ORDERS[q][1], off)
        for off in NEAR_FIRST:
            for q in range(nq):
                send(q * CROSS + 1, 6, (RING - off, 0), 6 * q, ORDERS[q][2], off)

    def send_row(r):
        for off in NEAR_FIRST:
            for q in range(nq):
                send(RUNS[(0, r)][0] + 3 * q, 3, (RING - off, r), 3 * q, ORDERS[q][2], off)

    for load in small + [doc_load]:
        load.wait()

    def document(rows, mask_row, out):
        limit = length(mask_row)
        head = None
        for c in range(dlen // CHUNK):
            part = pl.ds(c * CHUNK, CHUNK)
            y = project(rows[part, :])
            head = y[0:1, :] if head is None else head
            out[part, :] = jnp.where(row_ids(CHUNK, proj) + c * CHUNK < limit, y, head).astype(jnp.bfloat16)

    for j in range(nq):
        document(dv.at[j], dmv[j:j + 1, :], docs.at[core * nq + j])

    my_docs = docs.at[pl.ds(core * nq, nq)]
    their_docs = docs.at[pl.ds((1 - core) * nq, nq)]
    doc_send = remote(my_docs, my_docs, doc_sem.at[0], doc_sem.at[1], partner)
    doc_recv = remote(their_docs, their_docs, doc_sem.at[0], doc_sem.at[1], partner)
    contract = (((1,), (1,)), ((), ()))
    cell_row = lax.broadcasted_iota(jnp.int32, (8, proj), 0)
    cell_lane = lax.broadcasted_iota(jnp.int32, (8, proj), 1)
    cell = cell_row * proj + cell_lane

    def negative(i, k):
        if k == 0:
            neg_loads[i].wait()
        document(nv.at[i, k], nmv[i, k:k + 1, :], negs.at[i * nneg + k])

    def hard_scores():
        found = hard[...]
        for i in range(nq):
            mine = gath[i * CROSS]
            for k in range(nneg):
                sim = lax.dot_general(negs[i * nneg + k], mine, contract, preferred_element_type=jnp.float32)
                score = jnp.sum(jnp.max(sim, axis=0, keepdims=True), axis=1, keepdims=True)
                found = jnp.where((cell_row == i) & (cell_lane == k + 1), score, found)
        hard[...] = found

    def place(q, p, r, c):
        index = q
        for axis, steps in zip(reversed(ORDERS[q]), (p, r, c)):
            index = index * RING + (lax.rem(pos[axis] + steps, RING) if steps else pos[axis])
        return index

    tile = TILE * qlen
    tile_row = lax.broadcasted_iota(jnp.int32, (8, tile), 0)

    def segment(g):
        for n, t in enumerate(GROUPS[g]):
            rows = gath[t * TILE:(t + 1) * TILE].reshape(tile, proj)
            unit = jnp.zeros((8, tile), jnp.float32)
            for j in range(2 * nq):
                sim = lax.dot_general(docs[j], rows, contract, preferred_element_type=jnp.float32)
                unit = jnp.where(tile_row == j, jnp.max(sim, axis=0, keepdims=True), unit)
            best[g % 2, 2 * n] = unit[:, :proj]
            best[g % 2, 2 * n + 1] = unit[:, proj:]

    def reduce_segment(g):
        pieces = 2 * len(GROUPS[g])
        per = proj // qlen
        flat = best[g % 2, :pieces].reshape(pieces * 8, proj)
        high = flat.astype(jnp.bfloat16)
        left = flat - high.astype(jnp.float32)
        middle = left.astype(jnp.bfloat16)
        low = (left - middle.astype(jnp.float32)).astype(jnp.bfloat16)
        sums = jnp.dot(jnp.concatenate([high, middle, low], axis=0), ones[...], preferred_element_type=jnp.float32)
        size = pieces * 8
        scores = (sums[:size] + sums[size:2 * size] + sums[2 * size:]).reshape(pieces, 8, per * proj)
        real = lax.broadcasted_iota(jnp.int32, scores.shape, 1) < 2 * nq
        top = jnp.max(jnp.where(real, scores, LOW), axis=1, keepdims=True)
        mass = jnp.sum(jnp.where(real, jnp.exp((scores - top) / tau), 0.0), axis=1, keepdims=True)
        part = top / tau + jnp.log(mass)
        packed = dense[...]
        first = GROUPS[g][0] * TILE
        for b in range(pieces * per):
            values = lax.slice(part, (b // per, 0, b % per * proj), (b // per + 1, 1, (b % per + 1) * proj))[0]
            packed = jnp.where(cell == place(*BLOCKS[first + b]), values, packed)
        dense[...] = packed
        if g == 0:
            students = hard[...]
            for q in range(nq):
                b = q * CROSS
                column = lax.slice(scores, (b // per, 0, b % per * proj), (b // per + 1, 8, (b % per + 1) * proj))[0]
                hit = jnp.sum(jnp.where(cell_row == core * nq + q, column, 0.0), axis=0, keepdims=True)
                students = jnp.where((cell_row == q) & (cell_lane == 0), hit, students)
            hard[...] = students

    def log_softmax(z):
        z = z - jnp.max(z, axis=1, keepdims=True)
        return z - jnp.log(jnp.sum(jnp.exp(z), axis=1, keepdims=True))

    def finish_rows():
        logits = hard[:nq, :nneg + 1] / tau
        teacher_log = log_softmax(tev[...])
        student_log = log_softmax(logits)
        rest = jnp.sum(jnp.exp(teacher_log) * (teacher_log - student_log), axis=1, keepdims=True) - logits[:, 0:1]
        rest_ref[...] = jnp.broadcast_to(rest, rest_ref.shape)
        rest_sum = jnp.sum(rest, axis=0, keepdims=True)
        dense[...] = jnp.where((cell_row == 1) & (cell_lane == proj - 1), rest_sum, dense[...])

    negative(0, 0)
    doc_send.start()
    for n in range(1, EARLY):
        negative(n // nneg, n % nneg)
    arrived('cross')
    send_cross()
    for n in range(EARLY, nq * nneg):
        negative(n // nneg, n % nneg)
    hard_scores()
    doc_recv.wait_recv()
    waited = {'cross'}
    for g, group in enumerate(GROUPS):
        for name, (at, count) in RUNS.items():
            if at < (group[-1] + 1) * TILE and name not in waited:
                waited.add(name)
                arrived(name)
                if not name[0]:
                    send_row(name[1])
        if g:
            reduce_segment(g - 1)
        if g == 2:
            finish_rows()
        segment(g)
    reduce_segment(len(GROUPS) - 1)

    here = core * CHIPS + chip
    inbox[here] = dense[0:2, :]
    mine = inbox.at[here]
    for steps in OTHERS + [(0, 0, 0)]:
        for other in (0, 1):
            if other or any(steps):
                remote(mine, mine, osend, orecv, device(steps, other)).start()
    others = inbox.at[pl.ds(0, 2 * CHIPS - 1)]
    remote(others, others, osend, orecv, partner).wait_recv()

    r_id = lax.broadcasted_iota(jnp.int32, (2, proj), 0)
    l_id = lax.broadcasted_iota(jnp.int32, (2, proj), 1)
    r_cell = r_id * proj + l_id

    def merged(which):
        parts = inbox[pl.ds(which * CHIPS, CHIPS)]
        top = jnp.max(parts, axis=0)
        lse = top + jnp.log(jnp.sum(jnp.exp(parts - top[None]), axis=0))
        extra = jnp.where((r_id == 1) & (l_id == proj - 1), jnp.sum(parts, axis=0), 0.0)
        return lse, jnp.where(r_cell < nq * CHIPS, lse, extra)

    lse, total = merged(core)
    total = total + merged(1 - core)[1]
    values = jnp.where((cell_row == 0) & (cell_lane == nq), jnp.sum(jnp.sum(total, axis=0, keepdims=True), axis=1, keepdims=True) / (2 * CHIPS * nq), 0.0)
    for q in range(nq):
        spot = r_cell == place(q, 0, 0, 0)
        mine_q = jnp.sum(jnp.sum(jnp.where(spot, lse, 0.0), axis=0, keepdims=True), axis=1, keepdims=True) + rest_ref[q:q + 1, 0:1]
        values = jnp.where((cell_row == 0) & (cell_lane == q), mine_q, values)
    out_ref[...] = values

    doc_send.wait_send()
    remote(others, others, osend, orecv, partner).wait_send()
    sent = gath.at[pl.ds(0, len(BLOCKS) - nq)]
    remote(sent, sent, gsend, grecv.at[0], partner).wait_send()


def split(packed, loss_ref, mean_ref):
    for q in range(loss_ref.shape[0]):
        loss_ref[q] = packed[0, q]
    mean_ref[0] = packed[0, loss_ref.shape[0]]


def solution(mesh):
    batch_axes = ('replica', 'data')

    def local_loss(query_hidden, doc_hidden, neg_hidden, query_mask, doc_mask, neg_mask, teacher, w_proj, temperature):
        nq, qlen, width = query_hidden.shape
        dlen, nneg = doc_hidden.shape[1], neg_hidden.shape[1]
        proj = w_proj.shape[1]
        anywhere = pl.BlockSpec(memory_space=pl.ANY)
        smem = pl.BlockSpec(memory_space=pltpu.SMEM)
        rows = nq * (qlen + dlen + nneg * dlen)
        result = pl.pallas_call(
            kernel,
            name='late_interaction',
            out_shape=pltpu.VMEM((8, 128), jnp.float32),
            in_specs=[anywhere] * 8 + [smem],
            out_specs=pl.BlockSpec(memory_space=pltpu.VMEM),
            scratch_shapes=[
                pltpu.VMEM(query_hidden.shape, jnp.bfloat16),
                pltpu.VMEM(doc_hidden.shape, jnp.bfloat16),
                pltpu.VMEM(neg_hidden.shape, jnp.bfloat16),
                pltpu.VMEM(query_mask.shape, jnp.int32),
                pltpu.VMEM(doc_mask.shape, jnp.int32),
                pltpu.VMEM(neg_mask.shape, jnp.int32),
                pltpu.VMEM(teacher.shape, jnp.float32),
                pltpu.VMEM(w_proj.shape, jnp.bfloat16),
                pltpu.VMEM((len(BLOCKS), qlen, proj), jnp.bfloat16),
                pltpu.VMEM((2 * nq, dlen, proj), jnp.bfloat16),
                pltpu.VMEM((nq * nneg, dlen, proj), jnp.bfloat16),
                pltpu.VMEM((2, 2 * max(map(len, GROUPS)), 8, proj), jnp.float32),
                pltpu.VMEM((8, proj), jnp.float32),
                pltpu.VMEM((proj, proj // qlen * proj), jnp.bfloat16),
                pltpu.VMEM((8, proj), jnp.float32),
                pltpu.VMEM((nq, proj), jnp.float32),
                pltpu.VMEM((2 * CHIPS, 2, proj), jnp.float32),
                pltpu.SemaphoreType.DMA((7 + nq,)),
                pltpu.SemaphoreType.DMA((2,)),
                pltpu.SemaphoreType.DMA,
                pltpu.SemaphoreType.DMA((len(RUNS),)),
                pltpu.SemaphoreType.DMA,
                pltpu.SemaphoreType.DMA,
            ],
            compiler_params=pltpu.CompilerParams(
                collective_id=0, has_side_effects=True, vmem_limit_bytes=60 * 1024 * 1024),
            cost_estimate=pl.CostEstimate(
                flops=2 * proj * (rows * width + CHIPS * nq * qlen * 2 * nq * dlen),
                bytes_accessed=2 * rows * width, transcendentals=rows),
        )(query_hidden, doc_hidden, neg_hidden, query_mask, doc_mask, neg_mask, teacher, w_proj,
          temperature.reshape(1))
        return pl.pallas_call(
            split,
            name='split_results',
            out_shape=(jax.ShapeDtypeStruct((nq,), jnp.float32), jax.ShapeDtypeStruct((1,), jnp.float32)),
            in_specs=[pl.BlockSpec(memory_space=pltpu.VMEM)],
            out_specs=(smem, smem),
        )(pltpu.with_memory_space_constraint(result, pltpu.VMEM))

    in_specs = (P(batch_axes, None, None), P(batch_axes, None, None), P(batch_axes, None, None, None),
                P(batch_axes, None), P(batch_axes, None), P(batch_axes, None, None), P(batch_axes, None),
                P(None, None), P())
    out_specs = (P(batch_axes), P('replica'))
    return jax.shard_map(local_loss, mesh=mesh, in_specs=in_specs, out_specs=out_specs, check_vma=False)
```

```python
import jax
import jax.numpy as jnp
from jax import lax
from jax.experimental import pallas as pl
from jax.experimental.pallas import tpu as pltpu
from jax.sharding import PartitionSpec as P

RING = 4
CHIPS = RING ** 3
ORDERS = ((0, 2, 1), (1, 0, 2), (2, 1, 0))
NEAR_FIRST = (1, 3, 2)
STEPS = range(1, RING)
QUERIES = range(len(ORDERS))


def layout():
    runs, blocks = {}, []

    def add(name, members):
        runs[name] = (len(blocks), len(members))
        blocks.extend(members)

    add('cross', [b for q in QUERIES for b in
                  [(q, 0, 0, 0)] + [(q, 0, 0, c) for c in STEPS] + [(q, 0, r, 0) for r in STEPS]
                  + [(q, p, 0, 0) for p in STEPS]])
    for r in NEAR_FIRST:
        add((0, r), [(q, 0, r, c) for q in QUERIES for c in STEPS])
    for p in NEAR_FIRST:
        add((p, 0), [b for q in QUERIES for b in
                     [(q, p, 0, c) for c in STEPS] + [(q, p, r, 0) for r in STEPS]])
    for p, r in ((1, 1), (3, 1), (1, 3), (3, 3), (2, 1), (2, 3), (1, 2), (3, 2), (2, 2)):
        add((p, r), [(q, p, r, c) for q in QUERIES for c in STEPS])
    return runs, blocks


RUNS, BLOCKS = layout()
CROSS = len(BLOCKS[:RUNS['cross'][1]]) // len(ORDERS)
TILE = 8
GROUPS = ((0, 1, 2), (3, 4, 5, 6), (7, 8, 9), (10, 11, 12), (13, 14, 15), (16, 17, 18, 19), (20, 21, 22, 23))
OTHERS = sorted([(x, y, z) for x in range(RING) for y in range(RING) for z in range(RING) if x or y or z],
                key=lambda v: -sum(min(a, RING - a) for a in v))
LOW = -3.0e38
CHUNK = 256
EARLY = 6
MESH = pl.DeviceIdType.MESH


def kernel(qh, dh, nh, qm, dm, nm, te, w, tau_ref, out_ref,
           qv, dv, nv, qmv, dmv, nmv, tev, wv, gath, docs, negs, best, hard, ones, dense, rest_ref, inbox,
           in_sem, doc_sem, gsend, grecv, osend, orecv):
    me = lax.axis_index('data')
    core = lax.rem(me, 2)
    chip = me // 2
    pos = (lax.rem(chip, RING), lax.rem(chip // RING, RING), chip // (RING * RING))
    nq, dlen, width = dv.shape
    nneg, qlen, proj = nv.shape[1], qv.shape[1], wv.shape[1]
    tau = tau_ref[0]

    def device(steps, other=0):
        c = [lax.rem(pos[a] + steps[a], RING) if steps[a] else pos[a] for a in range(3)]
        return {'data': ((c[2] * RING + c[1]) * RING + c[0]) * 2 + (1 - core if other else core)}

    def along(axis, off):
        return device([off if a == axis else 0 for a in range(3)])

    partner = device((0, 0, 0), 1)

    def remote(src, dst, send, recv, target):
        return pltpu.make_async_remote_copy(src_ref=src, dst_ref=dst, send_sem=send, recv_sem=recv,
                                            device_id=target, device_id_type=MESH)

    pairs = ((w, wv), (qh, qv), (qm, qmv), (dm, dmv), (nm, nmv), (te, tev))
    loads = [pltpu.make_async_copy(src, dst, in_sem.at[n]) for n, (src, dst) in enumerate(pairs)]
    first, small = loads[:3], loads[3:]
    doc_load = pltpu.make_async_copy(dh, dv, in_sem.at[6])
    neg_loads = [pltpu.make_async_copy(nh.at[i], nv.at[i], in_sem.at[7 + i]) for i in range(nq)]
    for load in first + small + [doc_load] + neg_loads:
        load.start()

    barrier = pltpu.get_barrier_semaphore()
    for axis in range(3):
        for off in range(1, RING):
            pl.semaphore_signal(barrier, inc=1, device_id=along(axis, off), device_id_type=MESH)
    pl.semaphore_signal(barrier, inc=1, device_id=partner, device_id_type=MESH)

    def project(rows):
        y = jnp.dot(rows, wv[...], preferred_element_type=jnp.float32)
        return y * lax.rsqrt(jnp.sum(y * y, axis=-1, keepdims=True))

    def length(mask_row):
        return jnp.sum(mask_row.astype(jnp.float32), axis=-1, keepdims=True)

    def row_ids(rows, cols):
        return lax.broadcasted_iota(jnp.int32, (rows, cols), 0).astype(jnp.float32)

    hard[...] = jnp.zeros_like(hard)
    dense[...] = jnp.zeros_like(dense)
    e_row = lax.broadcasted_iota(jnp.int32, ones.shape, 0)
    e_from = lax.broadcasted_iota(jnp.int32, ones.shape, 1) // proj * qlen
    ones[...] = jnp.where((e_row >= e_from) & (e_row < e_from + qlen), 1.0, 0.0).astype(jnp.bfloat16)

    for load in first:
        load.wait()
    for q in range(nq):
        tok = project(qv[q])
        keep = row_ids(qlen, proj) < length(qmv[q:q + 1, :])
        gath[q * CROSS] = jnp.where(keep, tok, 0.0).astype(jnp.bfloat16)

    pl.semaphore_wait(barrier, 3 * (RING - 1) + 1)

    sems = {name: n for n, name in enumerate(RUNS)}

    def send(first, count, name, place_at, axis, off):
        at = RUNS[name][0] + place_at
        remote(gath.at[pl.ds(first, count)], gath.at[pl.ds(at, count)], gsend, grecv.at[sems[name]],
               along(axis, off)).start()

    def arrived(name):
        at, count = RUNS[name]
        part = gath.at[pl.ds(at, count if name != 'cross' else count - nq)]
        remote(part, part, gsend, grecv.at[sems[name]], partner).wait_recv()

    for off in NEAR_FIRST:
        for q in range(nq):
            for level in range(3):
                send(q * CROSS, 1, 'cross', q * CROSS + level * (RING - 1) + RING - off, ORDERS[q][level], off)

    def send_cross():
        for off in NEAR_FIRST:
            for q in range(nq):
                send(q * CROSS + 1, 3, (0, RING - off), 3 * q, ORDERS[q][1], off)
        for off in NEAR_FIRST:
            for q in range(nq):
                send(q * CROSS + 1, 6, (RING - off, 0), 6 * q, ORDERS[q][2], off)

    def send_row(r):
        for off in NEAR_FIRST:
            for q in range(nq):
                send(RUNS[(0, r)][0] + 3 * q, 3, (RING - off, r), 3 * q, ORDERS[q][2], off)

    for load in small + [doc_load]:
        load.wait()

    def document(rows, mask_row, out):
        limit = length(mask_row)
        head = None
        for c in range(dlen // CHUNK):
            part = pl.ds(c * CHUNK, CHUNK)
            y = project(rows[part, :])
            head = y[0:1, :] if head is None else head
            out[part, :] = jnp.where(row_ids(CHUNK, proj) + c * CHUNK < limit, y, head).astype(jnp.bfloat16)

    for j in range(nq):
        document(dv.at[j], dmv[j:j + 1, :], docs.at[core * nq + j])

    my_docs = docs.at[pl.ds(core * nq, nq)]
    their_docs = docs.at[pl.ds((1 - core) * nq, nq)]
    doc_send = remote(my_docs, my_docs, doc_sem.at[0], doc_sem.at[1], partner)
    doc_recv = remote(their_docs, their_docs, doc_sem.at[0], doc_sem.at[1], partner)
    contract = (((1,), (1,)), ((), ()))
    cell_row = lax.broadcasted_iota(jnp.int32, (8, proj), 0)
    cell_lane = lax.broadcasted_iota(jnp.int32, (8, proj), 1)
    cell = cell_row * proj + cell_lane

    def negative(i, k):
        if k == 0:
            neg_loads[i].wait()
        document(nv.at[i, k], nmv[i, k:k + 1, :], negs.at[i * nneg + k])

    def hard_scores():
        found = hard[...]
        for i in range(nq):
            mine = gath[i * CROSS]
            for k in range(nneg):
                sim = lax.dot_general(negs[i * nneg + k], mine, contract, preferred_element_type=jnp.float32)
                score = jnp.sum(jnp.max(sim, axis=0, keepdims=True), axis=1, keepdims=True)
                found = jnp.where((cell_row == i) & (cell_lane == k + 1), score, found)
        hard[...] = found

    def place(q, p, r, c):
        index = q
        for axis, steps in zip(reversed(ORDERS[q]), (p, r, c)):
            index = index * RING + (lax.rem(pos[axis] + steps, RING) if steps else pos[axis])
        return index

    tile = TILE * qlen
    tile_row = lax.broadcasted_iota(jnp.int32, (8, tile), 0)

    def segment(g):
        for n, t in enumerate(GROUPS[g]):
            rows = gath[t * TILE:(t + 1) * TILE].reshape(tile, proj)
            unit = jnp.zeros((8, tile), jnp.float32)
            for j in range(2 * nq):
                sim = lax.dot_general(docs[j], rows, contract, preferred_element_type=jnp.float32)
                unit = jnp.where(tile_row == j, jnp.max(sim, axis=0, keepdims=True), unit)
            best[g % 2, 2 * n] = unit[:, :proj]
            best[g % 2, 2 * n + 1] = unit[:, proj:]

    def reduce_segment(g):
        pieces = 2 * len(GROUPS[g])
        per = proj // qlen
        flat = best[g % 2, :pieces].reshape(pieces * 8, proj)
        high = flat.astype(jnp.bfloat16)
        left = flat - high.astype(jnp.float32)
        middle = left.astype(jnp.bfloat16)
        low = (left - middle.astype(jnp.float32)).astype(jnp.bfloat16)
        sums = jnp.dot(jnp.concatenate([high, middle, low], axis=0), ones[...], preferred_element_type=jnp.float32)
        size = pieces * 8
        scores = (sums[:size] + sums[size:2 * size] + sums[2 * size:]).reshape(pieces, 8, per * proj)
        real = lax.broadcasted_iota(jnp.int32, scores.shape, 1) < 2 * nq
        top = jnp.max(jnp.where(real, scores, LOW), axis=1, keepdims=True)
        mass = jnp.sum(jnp.where(real, jnp.exp((scores - top) / tau), 0.0), axis=1, keepdims=True)
        part = top / tau + jnp.log(mass)
        packed = dense[...]
        first = GROUPS[g][0] * TILE
        for b in range(pieces * per):
            values = lax.slice(part, (b // per, 0, b % per * proj), (b // per + 1, 1, (b % per + 1) * proj))[0]
            packed = jnp.where(cell == place(*BLOCKS[first + b]), values, packed)
        dense[...] = packed
        if g == 0:
            students = hard[...]
            for q in range(nq):
                b = q * CROSS
                column = lax.slice(scores, (b // per, 0, b % per * proj), (b // per + 1, 8, (b % per + 1) * proj))[0]
                hit = jnp.sum(jnp.where(cell_row == core * nq + q, column, 0.0), axis=0, keepdims=True)
                students = jnp.where((cell_row == q) & (cell_lane == 0), hit, students)
            hard[...] = students

    def log_softmax(z):
        z = z - jnp.max(z, axis=1, keepdims=True)
        return z - jnp.log(jnp.sum(jnp.exp(z), axis=1, keepdims=True))

    def finish_rows():
        logits = hard[:nq, :nneg + 1] / tau
        teacher_log = log_softmax(tev[...])
        student_log = log_softmax(logits)
        rest = jnp.sum(jnp.exp(teacher_log) * (teacher_log - student_log), axis=1, keepdims=True) - logits[:, 0:1]
        rest_ref[...] = jnp.broadcast_to(rest, rest_ref.shape)
        rest_sum = jnp.sum(rest, axis=0, keepdims=True)
        dense[...] = jnp.where((cell_row == 1) & (cell_lane == proj - 1), rest_sum, dense[...])

    negative(0, 0)
    doc_send.start()
    for n in range(1, EARLY):
        negative(n // nneg, n % nneg)
    arrived('cross')
    send_cross()
    for n in range(EARLY, nq * nneg):
        negative(n // nneg, n % nneg)
    hard_scores()
    doc_recv.wait_recv()
    waited = {'cross'}
    for g, group in enumerate(GROUPS):
        for name, (at, count) in RUNS.items():
            if at < (group[-1] + 1) * TILE and name not in waited:
                waited.add(name)
                arrived(name)
                if not name[0]:
                    send_row(name[1])
        if g:
            reduce_segment(g - 1)
        if g == 2:
            finish_rows()
        segment(g)
    reduce_segment(len(GROUPS) - 1)

    here = core * CHIPS + chip
    inbox[here] = dense[0:2, :]
    mine = inbox.at[here]
    for steps in OTHERS + [(0, 0, 0)]:
        for other in (1, 0):
            if other or any(steps):
                remote(mine, mine, osend, orecv, device(steps, other)).start()
    others = inbox.at[pl.ds(0, 2 * CHIPS - 1)]
    remote(others, others, osend, orecv, partner).wait_recv()

    r_id = lax.broadcasted_iota(jnp.int32, (2, proj), 0)
    l_id = lax.broadcasted_iota(jnp.int32, (2, proj), 1)
    r_cell = r_id * proj + l_id

    def merged(which):
        parts = inbox[pl.ds(which * CHIPS, CHIPS)]
        top = jnp.max(parts, axis=0)
        lse = top + jnp.log(jnp.sum(jnp.exp(parts - top[None]), axis=0))
        extra = jnp.where((r_id == 1) & (l_id == proj - 1), jnp.sum(parts, axis=0), 0.0)
        return lse, jnp.where(r_cell < nq * CHIPS, lse, extra)

    lse, total = merged(core)
    total = total + merged(1 - core)[1]
    values = jnp.where((cell_row == 0) & (cell_lane == nq), jnp.sum(jnp.sum(total, axis=0, keepdims=True), axis=1, keepdims=True) / (2 * CHIPS * nq), 0.0)
    for q in range(nq):
        spot = r_cell == place(q, 0, 0, 0)
        mine_q = jnp.sum(jnp.sum(jnp.where(spot, lse, 0.0), axis=0, keepdims=True), axis=1, keepdims=True) + rest_ref[q:q + 1, 0:1]
        values = jnp.where((cell_row == 0) & (cell_lane == q), mine_q, values)
    out_ref[...] = values

    doc_send.wait_send()
    remote(others, others, osend, orecv, partner).wait_send()
    sent = gath.at[pl.ds(0, len(BLOCKS) - nq)]
    remote(sent, sent, gsend, grecv.at[0], partner).wait_send()


def split(packed, loss_ref, mean_ref):
    count = loss_ref.shape[0]
    loss_ref[...] = packed[0, :count]
    mean_ref[...] = packed[0, count:count + 1]


def solution(mesh):
    batch_axes = ('replica', 'data')

    def local_loss(query_hidden, doc_hidden, neg_hidden, query_mask, doc_mask, neg_mask, teacher, w_proj, temperature):
        nq, qlen, width = query_hidden.shape
        dlen, nneg = doc_hidden.shape[1], neg_hidden.shape[1]
        proj = w_proj.shape[1]
        anywhere = pl.BlockSpec(memory_space=pl.ANY)
        smem = pl.BlockSpec(memory_space=pltpu.SMEM)
        rows = nq * (qlen + dlen + nneg * dlen)
        result = pl.pallas_call(
            kernel,
            name='late_interaction',
            out_shape=pltpu.VMEM((8, 128), jnp.float32),
            in_specs=[anywhere] * 8 + [smem],
            out_specs=pl.BlockSpec(memory_space=pltpu.VMEM),
            scratch_shapes=[
                pltpu.VMEM(query_hidden.shape, jnp.bfloat16),
                pltpu.VMEM(doc_hidden.shape, jnp.bfloat16),
                pltpu.VMEM(neg_hidden.shape, jnp.bfloat16),
                pltpu.VMEM(query_mask.shape, jnp.int32),
                pltpu.VMEM(doc_mask.shape, jnp.int32),
                pltpu.VMEM(neg_mask.shape, jnp.int32),
                pltpu.VMEM(teacher.shape, jnp.float32),
                pltpu.VMEM(w_proj.shape, jnp.bfloat16),
                pltpu.VMEM((len(BLOCKS), qlen, proj), jnp.bfloat16),
                pltpu.VMEM((2 * nq, dlen, proj), jnp.bfloat16),
                pltpu.VMEM((nq * nneg, dlen, proj), jnp.bfloat16),
                pltpu.VMEM((2, 2 * max(map(len, GROUPS)), 8, proj), jnp.float32),
                pltpu.VMEM((8, proj), jnp.float32),
                pltpu.VMEM((proj, proj // qlen * proj), jnp.bfloat16),
                pltpu.VMEM((8, proj), jnp.float32),
                pltpu.VMEM((nq, proj), jnp.float32),
                pltpu.VMEM((2 * CHIPS, 2, proj), jnp.float32),
                pltpu.SemaphoreType.DMA((7 + nq,)),
                pltpu.SemaphoreType.DMA((2,)),
                pltpu.SemaphoreType.DMA,
                pltpu.SemaphoreType.DMA((len(RUNS),)),
                pltpu.SemaphoreType.DMA,
                pltpu.SemaphoreType.DMA,
            ],
            compiler_params=pltpu.CompilerParams(
                collective_id=0, has_side_effects=True, vmem_limit_bytes=60 * 1024 * 1024),
            cost_estimate=pl.CostEstimate(
                flops=2 * proj * (rows * width + CHIPS * nq * qlen * 2 * nq * dlen),
                bytes_accessed=2 * rows * width, transcendentals=rows),
        )(query_hidden, doc_hidden, neg_hidden, query_mask, doc_mask, neg_mask, teacher, w_proj,
          temperature.reshape(1))
        return pl.pallas_call(
            split,
            name='split_results',
            out_shape=(jax.ShapeDtypeStruct((nq,), jnp.float32), jax.ShapeDtypeStruct((1,), jnp.float32)),
            in_specs=[pl.BlockSpec(memory_space=pltpu.VMEM)],
            out_specs=(pl.BlockSpec(memory_space=pltpu.VMEM),) * 2,
        )(pltpu.with_memory_space_constraint(result, pltpu.VMEM))

    in_specs = (P(batch_axes, None, None), P(batch_axes, None, None), P(batch_axes, None, None, None),
                P(batch_axes, None), P(batch_axes, None), P(batch_axes, None, None), P(batch_axes, None),
                P(None, None), P())
    out_specs = (P(batch_axes), P('replica'))
    return jax.shard_map(local_loss, mesh=mesh, in_specs=in_specs, out_specs=out_specs, check_vma=False)
```
